256 devices in a mesh: seq: 32 (over y, z_hi, core), head: 8 (over x, z_lo).
Axes of the slice: x: 4, y: 4, z: 8 (z_hi: 4, z_lo: 2; z = z_hi * 2 + z_lo), core: 2. Of those that a mesh axis runs over, the one named last changes fastest.
Arguments:
- queries: bfloat16 [512, 64, 128], P('seq', 'head'), may hold values from -5 to 5
- cache: bfloat16 [2, 2048, 8, 128, 128], P(None, 'seq', 'head'), may hold values from -5 to 5
- page_table: int32 [512, 64], replicated, may hold values from 0 to 2047, as said below
- page_count: int32 [512], replicated, may hold values from 32 to 64, as said below
- out_weight: bfloat16 [8192, 8192], P('head', 'seq'), may hold values from -0.0625 to 0.0625
Outputs:
- output: bfloat16 [512, 8192], P('head', 'seq')
The draws below stay inside these ranges and needn't reach their ends.
Inputs may be any that keep to these rules, and one draw needn't show every extreme that they name: `page_table`: within a row all 64 entries are distinct page ids; only the first page_count entries of a row are selected, the rest are arbitrary. In every row at most 4 entries lie in one aligned block of 64 page ids, and the first 4 entries of every row lie in one such block. `page_count`: some sequence has exactly 64 selected pages.
All inputs are finite; a program needn't handle non-finite values.
Results may differ from the reference program's by a relative error of at most 0.0095.
Values may be sent and summed in bfloat16 or wider, within the bound.
A program may use at most 128 MiB of HBM per device.

```python
import math
import jax
import jax.numpy as jnp
from jax import lax

D = 8192
QH = 64
KVH = 8
HD = 128
PAGE = 128
SEL = 64
CAP = 4
PAGES_DEV = 64
BATCH = 512
POOL = 2048


def draw_queries(key, part):
    values = jnp.clip(jax.random.normal(jax.random.fold_in(key, 1), (BATCH, QH, HD), jnp.float32), -5.0, 5.0)
    return values.astype(jnp.bfloat16)


def draw_cache(key, part):
    values = jnp.clip(jax.random.normal(jax.random.fold_in(key, 2), (2, POOL, KVH, PAGE, HD), jnp.float32), -5.0, 5.0)
    return values.astype(jnp.bfloat16)


def table_row(stream):
    blocks = POOL // PAGES_DEV
    first_block = jax.random.randint(jax.random.fold_in(stream, 1), (), 0, blocks)
    shuffled = jax.random.permutation(jax.random.fold_in(stream, 2), (blocks - 1) * CAP)
    others = (shuffled // CAP + first_block + 1) % blocks
    block_of = jnp.concatenate([jnp.full((CAP,), first_block, jnp.int32), others[:SEL - CAP].astype(jnp.int32)])
    position = jnp.arange(SEL, dtype=jnp.int32)
    earlier = (block_of[None, :] == block_of[:, None]) & (position[None, :] < position[:, None])
    rank = jnp.sum(earlier.astype(jnp.int32), axis=1)
    within = jax.random.permutation(jax.random.fold_in(stream, 3), PAGES_DEV).astype(jnp.int32)
    return block_of * PAGES_DEV + within[rank]


def draw_page_table(key, part):
    streams = jax.random.split(jax.random.fold_in(key, 21), BATCH)
    return jax.vmap(table_row)(streams).astype(jnp.int32)


def draw_page_count(key, part):
    counts = jax.random.randint(jax.random.fold_in(key, 22), (BATCH,), SEL // 2, SEL + 1)
    fullest = jax.random.randint(jax.random.fold_in(key, 23), (), 0, BATCH)
    return jnp.where(jnp.arange(BATCH, dtype=jnp.int32) == fullest, SEL, counts).astype(jnp.int32)


def levels(rng, dims, cuts, smallest, high):
    loudness = 1.0
    for axis_at, blocks in cuts:
        heights = jax.random.uniform(jax.random.fold_in(jax.random.fold_in(rng, 6), axis_at), (blocks,), jnp.float32, smallest / len(cuts), high / len(cuts))
        loudness = loudness * jnp.repeat(jnp.exp(heights), dims[axis_at] // blocks).reshape((-1,) + (1,) * (len(dims) - 1 - axis_at))
    return loudness


def normal_values(key, extent, width, bound, shards=(), kind=jnp.bfloat16):
    values = jax.random.normal(key, extent, jnp.float32) * width
    if len(shards) > 0:
        values = levels(key, extent, shards, -0.22, 0.18) * values
    return jnp.clip(values, min=-bound, max=bound).astype(kind)


def setup_inputs(seed: int = 0) -> dict:
    arg_keys = jax.random.split(jax.random.key(seed), 6)
    return {
        "queries": draw_queries(jax.random.fold_in(arg_keys[5], 71), 0),
        "cache": draw_cache(jax.random.fold_in(arg_keys[5], 71), 0),
        "page_table": draw_page_table(jax.random.fold_in(arg_keys[5], 71), 0),
        "page_count": draw_page_count(jax.random.fold_in(arg_keys[5], 71), 0),
        "out_weight": normal_values(arg_keys[4], (QH * HD, D), (QH * HD) ** -0.5, 0.0625, ((0, 8), (1, 32))),
    }


def reference(queries, cache, page_table, page_count, out_weight):
    group_size = QH // KVH
    score_scale = 1.0 / math.sqrt(HD)

    def attend_sequence(inputs):
        query, selected, counts = inputs
        key_pages = cache[0][selected].astype(jnp.float32)
        value_pages = cache[1][selected].astype(jnp.float32)
        grouped = query.reshape(KVH, group_size, HD).astype(jnp.float32)
        scores = jnp.einsum('kgd,pktd->kgpt', grouped, key_pages) * score_scale
        usable = (jnp.arange(SEL, dtype=jnp.int32) < counts)[None, None, :, None]
        scores = jnp.where(usable, scores, jnp.float32(-1e+30))
        largest = lax.optimization_barrier(jnp.max(scores, axis=(2, 3), keepdims=True))
        weights = jnp.where(usable, jnp.exp(scores - largest), jnp.float32(0.0))
        totals = lax.optimization_barrier(jnp.sum(weights, axis=(2, 3)))
        rounded = lax.optimization_barrier(weights.astype(jnp.bfloat16)).astype(jnp.float32)
        outputs = jnp.einsum('kgpt,pktd->kgd', rounded, value_pages)
        return (outputs / totals[:, :, None]).reshape(QH * HD).astype(jnp.bfloat16)
    attention = lax.map(attend_sequence, (queries, page_table, page_count))
    return jnp.dot(attention, out_weight, preferred_element_type=jnp.float32).astype(jnp.bfloat16)
```

```python
import functools
import math

import jax
import jax.numpy as jnp
from jax import lax
from jax.experimental import pallas as pl
from jax.experimental.pallas import tpu as pltpu
from jax.sharding import PartitionSpec as P

Y, Z, C = 4, 4, 2
BLOCKS = Y * Z * C
ROWS = 16
HEADS = 8
HD = 128
PAGE = 128
PAGES = 64
SLOTS = 64
BATCH = BLOCKS * ROWS
TILE = ROWS * HEADS
GROUPS = 8
LOWEST = -1024.0
LOG2E_SCALE = math.log2(math.e) / math.sqrt(HD)
F32, BF16 = jnp.float32, jnp.bfloat16
VMEM = pltpu.VMEM


def position():
    me = lax.axis_index("seq")
    return me // (Z * C), (me // C) % Z, me % C


def at_seq(y, z, c):
    return {"seq": (y * Z + z) * C + c}


def send(src, dst, send_sem, recv_sem, device):
    copy = pltpu.make_async_remote_copy(
        src_ref=src, dst_ref=dst, send_sem=send_sem, recv_sem=recv_sem,
        device_id=device, device_id_type=pl.DeviceIdType.MESH,
    )
    copy.start()
    return copy


def arrived(dst, send_sem, recv_sem, device):
    pltpu.make_async_remote_copy(
        src_ref=dst, dst_ref=dst, send_sem=send_sem, recv_sem=recv_sem,
        device_id=device, device_id_type=pl.DeviceIdType.MESH,
    ).wait_recv()


def seq_peers(y, z, c):
    peers = [at_seq(y, z, 1 - c)]
    peers += [at_seq(y, (z + d) % Z, c) for d in range(1, Z)]
    peers += [at_seq((y + d) % Y, z, c) for d in range(1, Y)]
    return peers


def greet(peers):
    barrier = pltpu.get_barrier_semaphore()
    for peer in peers:
        pl.semaphore_signal(barrier, inc=1, device_id=peer, device_id_type=pl.DeviceIdType.MESH)
    pl.semaphore_wait(barrier, len(peers))


class Gather:
    def __init__(self, buf, zs, zr, ys, yr, ds, dr):
        self.buf, self.sems = buf, (zs, zr, ys, yr, ds, dr)
        self.y, self.z, self.c = position()
        self.copies = []

    def spread(self, dz):
        y, z, c = self.y, self.z, self.c
        zs, zr, ys, yr, ds, dr = self.sems
        block = self.buf.at[y, (z - dz + Z) % Z, c]
        for dy in (2, 1, 3):
            self.copies.append(send(block, block, ys.at[dy, dz], yr.at[dy, dz], at_seq((y + dy) % Y, z, c)))
        self.copies.append(send(block, block, ds.at[0, dz], dr.at[0, dz], at_seq(y, z, 1 - c)))

    def start(self):
        y, z, c = self.y, self.z, self.c
        zs, zr, ys, yr, ds, dr = self.sems
        own = self.buf.at[y, z, c]
        for dz in (2, 1, 3):
            self.copies.append(send(own, own, zs.at[dz], zr.at[dz], at_seq(y, (z + dz) % Z, c)))
        self.spread(0)

    def from_z(self, dz):
        y, z, c = self.y, self.z, self.c
        zs, zr, ys, yr, ds, dr = self.sems
        arrived(self.buf.at[y, (z - dz + Z) % Z, c], zs.at[dz], zr.at[dz], at_seq(y, (z - dz + Z) % Z, c))
        self.spread(dz)

    def from_y(self, dy, dz):
        y, z, c = self.y, self.z, self.c
        zs, zr, ys, yr, ds, dr = self.sems
        block = self.buf.at[(y - dy + Y) % Y, (z - dz + Z) % Z, c]
        arrived(block, ys.at[dy, dz], yr.at[dy, dz], at_seq((y - dy + Y) % Y, z, c))
        self.copies.append(send(block, block, ds.at[dy, dz], dr.at[dy, dz], at_seq(y, z, 1 - c)))

    def from_core(self, dy, dz):
        y, z, c = self.y, self.z, self.c
        zs, zr, ys, yr, ds, dr = self.sems
        block = self.buf.at[(y - dy + Y) % Y, (z - dz + Z) % Z, 1 - c]
        arrived(block, ds.at[dy, dz], dr.at[dy, dz], at_seq(y, z, 1 - c))

    def finish(self):
        for copy in self.copies:
            copy.wait_send()


ORDER = [(0, 0)] + [(0, d) for d in (1, 3, 2)] + [(dy, dz) for dz in (0, 1, 3, 2) for dy in (1, 3, 2)]
GATHER_SEMS = [
    pltpu.SemaphoreType.DMA((Z,)), pltpu.SemaphoreType.DMA((Z,)),
    pltpu.SemaphoreType.DMA((Y, Z)), pltpu.SemaphoreType.DMA((Y, Z)),
    pltpu.SemaphoreType.DMA((Y, Z)), pltpu.SemaphoreType.DMA((Y, Z)),
]


def dot(a, b, dims=((1,), (0,))):
    return lax.dot_general(a, b, (dims, ((), ())), preferred_element_type=F32)


def selection(table, counts):
    own = lax.axis_index("seq")
    square = lambda n, f: f(lax.broadcasted_iota(jnp.int32, (n, n), 0), lax.broadcasted_iota(jnp.int32, (n, n), 1)).astype(F32).astype(BF16)
    eye = square(SLOTS, jnp.equal)
    block = dot(eye, (table // PAGES).astype(F32).astype(BF16), ((1,), (1,)))
    page = dot(eye, (table % PAGES).astype(F32).astype(BF16), ((1,), (1,)))
    slot = lax.broadcasted_iota(jnp.int32, (SLOTS, BATCH), 0)
    present = (slot < counts) & (block == own.astype(F32))
    rank = dot(square(SLOTS, jnp.greater_equal), present.astype(F32).astype(BF16))
    rows = [jnp.sum(jnp.where(present & (rank == k + 1.0), page + 1.0, 0.0), axis=0, keepdims=True) for k in range(4)]
    more = (rows[2] > 0.0).astype(F32)
    place = dot(jnp.broadcast_to(more, (8, BATCH)).astype(BF16), square(BATCH, jnp.less_equal))[0:1]
    total = jnp.sum(more, axis=1, keepdims=True)
    at = lax.broadcasted_iota(jnp.int32, (BATCH, BATCH), 0).astype(F32)
    onehot = jnp.where((at + 1.0 == place) & (more > 0.0), 1.0, 0.0).astype(BF16)
    who = lax.broadcasted_iota(jnp.int32, (8, BATCH), 1)
    high = dot((who // 16).astype(F32).astype(BF16), onehot, ((1,), (1,)))[0:1]
    low = dot((who % 16).astype(F32).astype(BF16), onehot, ((1,), (1,)))[0:1]
    number = lax.broadcasted_iota(jnp.int32, (1, BATCH), 1).astype(F32)
    many = jnp.where(number < total, high * 16.0 + low, float(BATCH))
    return jnp.concatenate(rows + [many, jnp.broadcast_to(total, (1, BATCH))] + [jnp.zeros((2, BATCH), F32)], axis=0).astype(jnp.int32)


def prepare_kernel(q_ref, table_ref, counts_ref, cache_ref, all_ref, pick_ref, kt_ref, keys, turned, key_sems, out_sem, *sems):
    y, z, c = position()
    quarter = PAGES // 4
    loads = [
        pltpu.make_async_copy(cache_ref.at[0, pl.ds(i * quarter, quarter)], keys.at[pl.ds(i * quarter, quarter)], key_sems.at[i])
        for i in range(4)
    ]
    for load in loads:
        load.start()
    greet(seq_peers(y, z, c))
    all_ref[y, z, c] = q_ref[...]
    gather = Gather(all_ref, *sems)
    gather.start()
    pick_ref[...] = selection(table_ref[...], counts_ref[...])

    def turn(i, carry):
        for j in range(4):
            turned[i * 4 + j] = keys[i * 4 + j].T
        return carry

    loads[0].wait()
    loads[1].wait()
    lax.fori_loop(0, 8, turn, 0)
    for dz in (1, 3, 2):
        gather.from_z(dz)
    loads[2].wait()
    loads[3].wait()
    lax.fori_loop(8, 16, turn, 0)
    out = pltpu.make_async_copy(turned, kt_ref, out_sem)
    out.start()
    for dy, dz in ORDER[4:]:
        gather.from_y(dy, dz)
    for dy, dz in ORDER:
        gather.from_core(dy, dz)
    gather.finish()
    out.wait()


def prepare(q, table, counts, cache):
    vmem = pl.BlockSpec(memory_space=VMEM)
    return pl.pallas_call(
        prepare_kernel,
        out_shape=(
            jax.ShapeDtypeStruct((Y, Z, C, TILE, HD), BF16),
            jax.ShapeDtypeStruct((8, BATCH), jnp.int32),
            jax.ShapeDtypeStruct((PAGES, HD, PAGE), BF16),
        ),
        in_specs=[vmem, vmem, vmem, pl.BlockSpec(memory_space=pl.ANY)],
        out_specs=(vmem, vmem, pl.BlockSpec(memory_space=pl.ANY)),
        scratch_shapes=[
            VMEM((PAGES, PAGE, HD), BF16),
            VMEM((PAGES, HD, PAGE), BF16),
            pltpu.SemaphoreType.DMA((4,)),
            pltpu.SemaphoreType.DMA,
            *GATHER_SEMS,
        ],
        compiler_params=pltpu.CompilerParams(collective_id=0, has_side_effects=True, vmem_limit_bytes=32 << 20),
        name="prepare",
    )(q, table, counts, cache)


def attend_kernel(pick, q_in, kt_in, cache_ref, acc_out, stats_out, kt, v, q, scores, acc, top, total, kt_sem, v_sem):
    load_kt = pltpu.make_async_copy(kt_in, kt, kt_sem)
    load_v = pltpu.make_async_copy(cache_ref.at[1], v, v_sem)
    load_kt.start()
    load_v.start()

    def widen(i, carry):
        for j in range(4):
            q[pl.ds((i * 4 + j) * ROWS, ROWS)] = q_in[i * 4 + j].astype(F32).reshape(ROWS, HEADS, HD)
        return carry

    lax.fori_loop(0, BLOCKS // 4, widen, 0)
    q[pl.ds(BATCH, 8)] = jnp.zeros((8, HEADS, HD), F32)
    load_kt.wait()
    zeros = jnp.zeros((HEADS, HD), F32)

    def pages_of(b, first):
        safe = jnp.minimum(b, BATCH - 1)
        picks = [pick[first, safe], pick[first + 1, safe]]
        return [jnp.maximum(p - 1, 0) for p in picks], [jnp.where(p > 0, 0.0, -1e30).astype(F32) for p in picks]

    def score(a, b, first):
        pa, _ = pages_of(a, first)
        pb, _ = pages_of(b, first)
        left = jnp.concatenate(
            [jnp.concatenate([q[a], zeros], axis=1), jnp.concatenate([zeros, q[b]], axis=1)], axis=0
        ).astype(BF16)
        right = jnp.concatenate(
            [jnp.concatenate([kt[pa[0]], kt[pa[1]]], axis=1), jnp.concatenate([kt[pb[0]], kt[pb[1]]], axis=1)], axis=0
        )
        return dot(left, right)

    def weigh(s, b, first):
        _, bias = pages_of(b, first)
        s0 = s[:, :PAGE] * LOG2E_SCALE + bias[0]
        s1 = s[:, PAGE:] * LOG2E_SCALE + bias[1]
        highest = jnp.max(jnp.maximum(s0, s1), axis=1, keepdims=True)
        m = jnp.maximum(jnp.floor(highest * 0.5 + 0.5) * 2.0, LOWEST)
        w0, w1 = jnp.exp2(s0 - m), jnp.exp2(s1 - m)
        return m, jnp.sum(w0 + w1, axis=1, keepdims=True), jnp.concatenate([w0, w1], axis=1)

    def attend(s, a, b, first):
        pa, _ = pages_of(a, first)
        pb, _ = pages_of(b, first)
        ma, la, wa = weigh(s[:HEADS], a, first)
        mb, lb, wb = weigh(s[HEADS:], b, first)
        weights = jnp.concatenate([wa, wb], axis=0).astype(BF16)
        right = jnp.concatenate(
            [jnp.concatenate([v[pa[0]], v[pb[0]]], axis=1), jnp.concatenate([v[pa[1]], v[pb[1]]], axis=1)], axis=0
        )
        o = dot(weights, right)
        return (ma, la, o[:HEADS, :HD]), (mb, lb, o[HEADS:, HD:])

    units = ROWS // 2

    def scores_of(g):
        for u in range(units):
            b = g * ROWS + 2 * u
            scores[u] = score(b, b + 1, 0)

    scores_of(0)
    load_v.wait()

    def step(g, carry):
        for u in range(units):
            b = g * ROWS + 2 * u
            for k, (m, l, o) in enumerate(attend(scores[u], b, b + 1, 0)):
                acc[b + k] = o
                top[b + k] = jnp.broadcast_to(m, (HEADS, HD))
                total[b + k] = jnp.broadcast_to(l, (HEADS, HD))
        scores_of(jnp.minimum(g + 1, BLOCKS - 1))
        return carry

    lax.fori_loop(0, BLOCKS, step, 0)
    many = pick[5, 0]

    def more(i, carry):
        whose = [pick[4, i * ROWS + j] for j in range(ROWS)]
        for u in range(units):
            a, b = whose[2 * u], whose[2 * u + 1]
            for who, (m, l, o) in zip((a, b), attend(score(a, b, 2), a, b, 2)):
                m0 = top[who]
                m1 = jnp.maximum(m0, m)
                f0, f1 = jnp.exp2(m0 - m1), jnp.exp2(m - m1)
                acc[who] = acc[who] * f0 + o * f1
                total[who] = total[who] * f0 + l * f1
                top[who] = m1
        return carry

    lax.fori_loop(0, (many + ROWS - 1) // ROWS, more, 0)
    sublane = lax.broadcasted_iota(jnp.int32, (HEADS, HD), 0)
    lane = lax.broadcasted_iota(jnp.int32, (HEADS, HD), 1)

    def close(g, carry):
        tops = jnp.zeros((HEADS, HD), F32)
        totals = jnp.zeros((HEADS, HD), F32)
        for s in range(ROWS):
            here = lane - sublane == s * HEADS
            tops = jnp.where(here, top[g * ROWS + s], tops)
            totals = jnp.where(here, total[g * ROWS + s], totals)
        stats_out[g, 0:1] = jnp.sum(tops, axis=0, keepdims=True)
        stats_out[g, 1:2] = jnp.sum(totals, axis=0, keepdims=True)
        acc_out[g] = acc[pl.ds(g * ROWS, ROWS)].reshape(TILE, HD).astype(BF16)
        return carry

    lax.fori_loop(0, BLOCKS, close, 0)


def attend(pick, q, kt, cache):
    vmem = pl.BlockSpec(memory_space=VMEM)
    hbm = pl.BlockSpec(memory_space=pl.ANY)
    return pl.pallas_call(
        attend_kernel,
        out_shape=(
            jax.ShapeDtypeStruct((BLOCKS, TILE, HD), BF16),
            jax.ShapeDtypeStruct((BLOCKS, 2, HD), F32),
        ),
        in_specs=[pl.BlockSpec(memory_space=pltpu.SMEM), vmem, hbm, hbm],
        out_specs=(vmem, vmem),
        scratch_shapes=[
            VMEM((PAGES, HD, PAGE), BF16),
            VMEM((PAGES, PAGE, HD), BF16),
            VMEM((BATCH + 8, HEADS, HD), F32),
            VMEM((ROWS // 2, 2 * HEADS, 2 * PAGE), F32),
            VMEM((BATCH + 8, HEADS, HD), F32),
            VMEM((BATCH + 8, HEADS, HD), F32),
            VMEM((BATCH + 8, HEADS, HD), F32),
            pltpu.SemaphoreType.DMA,
            pltpu.SemaphoreType.DMA,
        ],
        compiler_params=pltpu.CompilerParams(vmem_limit_bytes=40 << 20),
        name="attend",
    )(pick, q, kt, cache)


def merge(parts, stats, diagonal):
    m = functools.reduce(jnp.maximum, [s[0:1] for s in stats])
    factors = [jnp.exp2(s[0:1] - m) for s in stats]
    total = sum(s[1:2] * f for s, f in zip(stats, factors))
    left = jnp.concatenate([jnp.where(diagonal, jnp.broadcast_to(f, (TILE, TILE)), 0.0).astype(BF16) for f in factors], axis=1)
    return dot(left, jnp.concatenate(parts, axis=0)), m, total


def finish_kernel(
    acc, stats, w_ref, out_ref,
    core_acc, core_stats, y_out, y_out_stats, y_in, y_in_stats, z_out, z_out_stats, z_in, z_in_stats,
    turned, att, w, part, parts_in, w_sem,
    c_send, c_recv, cs_send, cs_recv, y_send, y_recv, ys_send, ys_recv, z_send, z_recv, zs_send, zs_recv, h_send, h_recv, *sems,
):
    y, z, c = position()
    h = lax.axis_index("head")
    other = 1 - c
    load_w = pltpu.make_async_copy(w_ref, w, w_sem)
    load_w.start()
    greet(seq_peers(y, z, c) + [{"head": (h + d) % GROUPS} for d in range(1, GROUPS)])
    copies = []
    partner = at_seq(y, z, other)
    yorder = (2, 1, 3, 0)
    for d in yorder:
        yy = (y + d) % Y
        copies.append(send(acc.at[yy, :, other], core_acc.at[yy], c_send.at[d], c_recv.at[d], partner))
        copies.append(send(stats.at[yy, :, other], core_stats.at[yy], cs_send.at[d], cs_recv.at[d], partner))
    diagonal = lax.broadcasted_iota(jnp.int32, (TILE, TILE), 0) == lax.broadcasted_iota(jnp.int32, (TILE, TILE), 1)

    for d in yorder:
        yy = (y + d) % Y
        arrived(core_acc.at[yy], c_send.at[d], c_recv.at[d], partner)
        arrived(core_stats.at[yy], cs_send.at[d], cs_recv.at[d], partner)
        for i in range(Z):
            o, m, total = merge([acc[yy, i, c], core_acc[yy, i]], [stats[yy, i, c], core_stats[yy, i]], diagonal)
            if d == 0:
                y_in[0, i] = o.astype(BF16)
                y_in_stats[0, i, 0:1] = m
                y_in_stats[0, i, 1:2] = total
            else:
                y_out[d, i] = o.astype(BF16)
                y_out_stats[d, i, 0:1] = m
                y_out_stats[d, i, 1:2] = total
        if d != 0:
            there = at_seq(yy, z, c)
            copies.append(send(y_out.at[d], y_in.at[d], y_send.at[d], y_recv.at[d], there))
            copies.append(send(y_out_stats.at[d], y_in_stats.at[d], ys_send.at[d], ys_recv.at[d], there))
    for d in (1, 3, 2):
        there = at_seq((y - d + Y) % Y, z, c)
        arrived(y_in.at[d], y_send.at[d], y_recv.at[d], there)
        arrived(y_in_stats.at[d], ys_send.at[d], ys_recv.at[d], there)
    for d in (2, 1, 3, 0):
        zz = (z + d) % Z
        o, m, total = merge([y_in[i, zz] for i in range(Y)], [y_in_stats[i, zz] for i in range(Y)], diagonal)
        if d == 0:
            z_in[0] = o.astype(BF16)
            z_in_stats[0, 0:1] = m
            z_in_stats[0, 1:2] = total
        else:
            z_out[d] = o.astype(BF16)
            z_out_stats[d, 0:1] = m
            z_out_stats[d, 1:2] = total
            there = at_seq(y, zz, c)
            copies.append(send(z_out.at[d], z_in.at[d], z_send.at[d], z_recv.at[d], there))
            copies.append(send(z_out_stats.at[d], z_in_stats.at[d], zs_send.at[d], zs_recv.at[d], there))
    for d in (1, 3, 2):
        there = at_seq(y, (z - d + Z) % Z, c)
        arrived(z_in.at[d], z_send.at[d], z_recv.at[d], there)
        arrived(z_in_stats.at[d], zs_send.at[d], zs_recv.at[d], there)
    o, m, total = merge([z_in[i] for i in range(Z)], [z_in_stats[i] for i in range(Z)], diagonal)
    turned[...] = o / jnp.broadcast_to(total, (TILE, TILE)).T
    for i in range(HEADS):
        att[y, z, c, :, i * HD : (i + 1) * HD] = turned[pl.ds(i, ROWS, stride=HEADS), :].astype(BF16)
    gather = Gather(att, *sems)
    gather.start()
    for dz in (1, 3, 2):
        gather.from_z(dz)
    for dy, dz in ORDER[4:]:
        gather.from_y(dy, dz)
    for dy, dz in ORDER:
        gather.from_core(dy, dz)
    load_w.wait()
    for d in (4, 2, 6, 3, 5, 1, 7, 0):
        hh = (h + d) % GROUPS
        rows = jnp.concatenate([att[hh // 2, (hh % 2) * 2 + i, j] for i in range(2) for j in range(C)], axis=0)
        share = dot(rows, w[...]).astype(BF16)
        if d == 0:
            parts_in[0] = share
        else:
            part[d] = share
            copies.append(send(part.at[d], parts_in.at[d], h_send.at[d], h_recv.at[d], {"head": hh}))
    for d in (1, 7, 2, 6, 3, 5, 4):
        arrived(parts_in.at[d], h_send.at[d], h_recv.at[d], {"head": (h - d + GROUPS) % GROUPS})
    out_ref[...] = sum(parts_in[d].astype(F32) for d in range(GROUPS)).astype(BF16)
    gather.finish()
    for copy in copies:
        copy.wait_send()


def finish(acc, stats, w):
    vmem = pl.BlockSpec(memory_space=VMEM)
    width = w.shape[1]
    rows = BATCH // GROUPS
    dma = pltpu.SemaphoreType.DMA
    return pl.pallas_call(
        finish_kernel,
        out_shape=jax.ShapeDtypeStruct((rows, width), BF16),
        in_specs=[vmem, vmem, pl.BlockSpec(memory_space=pl.ANY)],
        out_specs=vmem,
        scratch_shapes=[
            VMEM((Y, Z, TILE, HD), BF16), VMEM((Y, Z, 2, HD), F32),
            VMEM((Y, Z, TILE, HD), BF16), VMEM((Y, Z, 2, HD), F32),
            VMEM((Y, Z, TILE, HD), BF16), VMEM((Y, Z, 2, HD), F32),
            VMEM((Z, TILE, HD), BF16), VMEM((Z, 2, HD), F32),
            VMEM((Z, TILE, HD), BF16), VMEM((Z, 2, HD), F32),
            VMEM((TILE, HD), F32),
            VMEM((Y, Z, C, ROWS, HEADS * HD), BF16),
            VMEM((HEADS * HD, width), BF16),
            VMEM((GROUPS, rows, width), BF16), VMEM((GROUPS, rows, width), BF16),
            dma,
            *[dma((Y,)) for _ in range(12)],
            dma((GROUPS,)), dma((GROUPS,)),
            *GATHER_SEMS,
        ],
        compiler_params=pltpu.CompilerParams(collective_id=1, has_side_effects=True, vmem_limit_bytes=32 << 20),
        name="finish",
    )(acc, stats, w)


def shards(queries, cache, page_table, page_count, out_weight):
    cache = cache.reshape(2, PAGES, PAGE, HD)
    q, pick, kt = prepare(queries.reshape(TILE, HD), page_table, page_count.reshape(1, BATCH), cache)
    acc, stats = attend(pick, q.reshape(BLOCKS, TILE, HD), kt, cache)
    return finish(acc.reshape(Y, Z, C, TILE, HD), stats.reshape(Y, Z, C, 2, HD), out_weight)


def solution(mesh):
    return jax.shard_map(
        shards,
        mesh=mesh,
        in_specs=(
            P("seq", "head", None),
            P(None, "seq", "head", None, None),
            P(),
            P(),
            P("head", "seq"),
        ),
        out_specs=P("head", "seq"),
        check_vma=False,
    )
```

```python
import functools
import math

import jax
import jax.numpy as jnp
from jax import lax
from jax.experimental import pallas as pl
from jax.experimental.pallas import tpu as pltpu
from jax.sharding import PartitionSpec as P

Y, Z, C = 4, 4, 2
BLOCKS = Y * Z * C
ROWS = 16
HEADS = 8
HD = 128
PAGE = 128
PAGES = 64
SLOTS = 64
BATCH = BLOCKS * ROWS
TILE = ROWS * HEADS
GROUPS = 8
CAP = 4
CHUNK = 8
UNROLL = 8
NONE = 2560
STEPS = NONE // CHUNK // UNROLL
LOWEST = -1000.0
LOG2E_SCALE = math.log2(math.e) / math.sqrt(HD)
F32, BF16 = jnp.float32, jnp.bfloat16
VMEM = pltpu.VMEM


def position():
    me = lax.axis_index("seq")
    return me // (Z * C), (me // C) % Z, me % C


def at_seq(y, z, c):
    return {"seq": (y * Z + z) * C + c}


def send(src, dst, send_sem, recv_sem, device):
    copy = pltpu.make_async_remote_copy(
        src_ref=src, dst_ref=dst, send_sem=send_sem, recv_sem=recv_sem,
        device_id=device, device_id_type=pl.DeviceIdType.MESH,
    )
    copy.start()
    return copy


def arrived(dst, send_sem, recv_sem, device):
    pltpu.make_async_remote_copy(
        src_ref=dst, dst_ref=dst, send_sem=send_sem, recv_sem=recv_sem,
        device_id=device, device_id_type=pl.DeviceIdType.MESH,
    ).wait_recv()


def seq_peers(y, z, c):
    peers = [at_seq(y, z, 1 - c)]
    peers += [at_seq(y, (z + d) % Z, c) for d in range(1, Z)]
    peers += [at_seq((y + d) % Y, z, c) for d in range(1, Y)]
    return peers


def greet(peers):
    barrier = pltpu.get_barrier_semaphore()
    for peer in peers:
        pl.semaphore_signal(barrier, inc=1, device_id=peer, device_id_type=pl.DeviceIdType.MESH)
    pl.semaphore_wait(barrier, len(peers))


class Gather:
    def __init__(self, buf, zs, zr, ys, yr, ds, dr):
        self.buf, self.sems = buf, (zs, zr, ys, yr, ds, dr)
        self.y, self.z, self.c = position()
        self.copies = []

    def spread(self, dz):
        y, z, c = self.y, self.z, self.c
        zs, zr, ys, yr, ds, dr = self.sems
        block = self.buf.at[y, (z - dz + Z) % Z, c]
        for dy in (2, 1, 3):
            self.copies.append(send(block, block, ys.at[dy, dz], yr.at[dy, dz], at_seq((y + dy) % Y, z, c)))
        self.copies.append(send(block, block, ds.at[0, dz], dr.at[0, dz], at_seq(y, z, 1 - c)))

    def start(self):
        y, z, c = self.y, self.z, self.c
        zs, zr, ys, yr, ds, dr = self.sems
        own = self.buf.at[y, z, c]
        for dz in (2, 1, 3):
            self.copies.append(send(own, own, zs.at[dz], zr.at[dz], at_seq(y, (z + dz) % Z, c)))
        self.spread(0)

    def from_z(self, dz):
        y, z, c = self.y, self.z, self.c
        zs, zr, ys, yr, ds, dr = self.sems
        arrived(self.buf.at[y, (z - dz + Z) % Z, c], zs.at[dz], zr.at[dz], at_seq(y, (z - dz + Z) % Z, c))
        self.spread(dz)

    def from_y(self, dy, dz):
        y, z, c = self.y, self.z, self.c
        zs, zr, ys, yr, ds, dr = self.sems
        block = self.buf.at[(y - dy + Y) % Y, (z - dz + Z) % Z, c]
        arrived(block, ys.at[dy, dz], yr.at[dy, dz], at_seq((y - dy + Y) % Y, z, c))
        self.copies.append(send(block, block, ds.at[dy, dz], dr.at[dy, dz], at_seq(y, z, 1 - c)))

    def from_core(self, dy, dz):
        y, z, c = self.y, self.z, self.c
        zs, zr, ys, yr, ds, dr = self.sems
        block = self.buf.at[(y - dy + Y) % Y, (z - dz + Z) % Z, 1 - c]
        arrived(block, ds.at[dy, dz], dr.at[dy, dz], at_seq(y, z, 1 - c))

    def finish(self):
        for copy in self.copies:
            copy.wait_send()


ORDER = [(0, 0)] + [(0, d) for d in (1, 3, 2)] + [(dy, dz) for dz in (0, 1, 3, 2) for dy in (1, 3, 2)]
GATHER_SEMS = [
    pltpu.SemaphoreType.DMA((Z,)), pltpu.SemaphoreType.DMA((Z,)),
    pltpu.SemaphoreType.DMA((Y, Z)), pltpu.SemaphoreType.DMA((Y, Z)),
    pltpu.SemaphoreType.DMA((Y, Z)), pltpu.SemaphoreType.DMA((Y, Z)),
]


def dot(a, b, dims=((1,), (0,))):
    return lax.dot_general(a, b, (dims, ((), ())), preferred_element_type=F32)


def square(n, f):
    return f(lax.broadcasted_iota(jnp.int32, (n, n), 0), lax.broadcasted_iota(jnp.int32, (n, n), 1)).astype(F32).astype(BF16)


def selection(table, counts):
    own = lax.axis_index("seq")
    page = (table % PAGES).astype(F32)
    slot = lax.broadcasted_iota(jnp.int32, (SLOTS, BATCH), 0)
    present = (slot < counts) & (table // PAGES == own)
    rank = dot(square(SLOTS, jnp.greater_equal), present.astype(F32).astype(BF16))
    picks = [jnp.sum(jnp.where(present & (rank == k + 1.0), page + 1.0, 0.0), axis=0, keepdims=True) for k in range(CAP)]
    number = lax.broadcasted_iota(jnp.int32, (PAGES, BATCH), 0).astype(F32)
    takes = [number + 1.0 == pick for pick in picks]
    taken = sum(take.astype(F32) for take in takes)
    before = dot(taken.astype(BF16), square(BATCH, jnp.less_equal))
    chunks = jnp.floor((jnp.sum(taken, axis=1, keepdims=True) + (CHUNK - 1.0)) * (1.0 / CHUNK))
    first = dot(square(PAGES, jnp.greater), jnp.broadcast_to(chunks, (PAGES, 128)).astype(BF16))[:, 0:1]
    place = first * CHUNK + before - 1.0
    places = [
        jnp.where(pick > 0.0, jnp.sum(jnp.where(take, place, 0.0), axis=0, keepdims=True), float(NONE))
        for pick, take in zip(picks, takes)
    ]
    total = jnp.sum(chunks, axis=0, keepdims=True)
    group = lax.broadcasted_iota(jnp.int32, (BLOCKS, BATCH), 0)
    mine = group == lax.broadcasted_iota(jnp.int32, (BLOCKS, BATCH), 1) // ROWS
    column = lax.broadcasted_iota(jnp.int32, (BATCH, 128), 1)
    within = lax.broadcasted_iota(jnp.int32, (BATCH, 128), 0) % ROWS
    high = jnp.zeros((BLOCKS, 128), F32)
    low = jnp.zeros((BLOCKS, 128), F32)
    for k, p in enumerate(places):
        put = (column == k * ROWS + within).astype(F32).astype(BF16)
        upper = jnp.floor(p * (1.0 / 16.0))
        high += dot(jnp.where(mine, upper, 0.0).astype(BF16), put)
        low += dot(jnp.where(mine, p - upper * 16.0, 0.0).astype(BF16), put)
    lane = lax.broadcasted_iota(jnp.int32, (BLOCKS, 128), 1)
    pick = jnp.where(lane == CAP * ROWS, total, high * 16.0 + low)
    chunk = lax.broadcasted_iota(jnp.int32, (PAGES, BATCH), 1).astype(F32)
    page_of = jnp.sum(jnp.where((first <= chunk) & (chunk < first + chunks), number, 0.0), axis=0, keepdims=True)
    step = lax.broadcasted_iota(jnp.int32, (STEPS, BATCH), 0)
    its = step == lax.broadcasted_iota(jnp.int32, (STEPS, BATCH), 1) // UNROLL
    put = (column == 64 + lax.broadcasted_iota(jnp.int32, (BATCH, 128), 0) % UNROLL).astype(F32).astype(BF16)
    pages = dot(jnp.where(its, page_of, 0.0).astype(BF16), put)
    return places, pick.astype(jnp.int32), pages.astype(jnp.int32)


def owners(places, start):
    at = lax.broadcasted_iota(jnp.int32, (256, BATCH), 0).astype(F32) + start.astype(F32)
    hit = (at == places[0:1]) | (at == places[1:2]) | (at == places[2:3]) | (at == places[3:4])
    who = lax.broadcasted_iota(jnp.int32, (8, BATCH), 1)
    digit = jnp.where(lax.broadcasted_iota(jnp.int32, (8, BATCH), 0) == 0, who // 16, who % 16)
    digits = dot(digit.astype(F32).astype(BF16), jnp.where(hit, 1.0, 0.0).astype(BF16), ((1,), (1,)))
    return (digits[0:1] * 16.0 + digits[1:2]).astype(jnp.int32)


def prepare_kernel(
    q_ref, table_ref, counts_ref, cache_ref, all_ref, pick_ref, who_ref, kt_ref, v_ref,
    table, counts, keys, places, pages, in_sems, key_sems, *sems,
):
    y, z, c = position()
    half = PAGES // 2
    small = [
        pltpu.make_async_copy(q_ref, all_ref.at[y, z, c], in_sems.at[0]),
        pltpu.make_async_copy(table_ref, table, in_sems.at[1]),
        pltpu.make_async_copy(counts_ref, counts, in_sems.at[2]),
    ]
    loads = [
        pltpu.make_async_copy(cache_ref.at[0, pl.ds(i * half, half)], keys.at[pl.ds(i * half, half)], key_sems.at[i])
        for i in range(2)
    ]
    load_v = pltpu.make_async_copy(cache_ref.at[1], v_ref, in_sems.at[3])
    for load in small + loads:
        load.start()
    greet(seq_peers(y, z, c))
    small[0].wait()
    gather = Gather(all_ref, *sems)
    gather.start()
    load_v.start()
    small[1].wait()
    small[2].wait()
    rows, pick_ref[...], pages[...] = selection(table[...], counts[...])
    for k in range(CAP):
        places[k : k + 1] = rows[k]

    def turn(i, carry):
        for j in range(4):
            kt_ref[i * 4 + j] = keys[i * 4 + j].T
        return carry

    def name(i, carry):
        lane = lax.broadcasted_iota(jnp.int32, (1, 128), 1)
        who = owners(places, i * 256)
        for j in range(2):
            half_row = who[:, j * 128 : (j + 1) * 128]
            rolled = pltpu.roll(jnp.broadcast_to(half_row, (8, 128)), 64, 1)[0:1]
            row = 4 * i + 2 * j
            who_ref[pl.ds(row, 1)] = jnp.where(lane < 64, half_row, pages[pl.ds(row, 1)])
            who_ref[pl.ds(row + 1, 1)] = jnp.where(lane < 64, rolled, pages[pl.ds(row + 1, 1)])
        return carry

    loads[0].wait()
    lax.fori_loop(0, 8, turn, 0)
    for dz in (1, 3, 2):
        gather.from_z(dz)
    loads[1].wait()
    lax.fori_loop(8, 16, turn, 0)
    lax.fori_loop(0, NONE // 256, name, 0)
    for dy, dz in ORDER[4:]:
        gather.from_y(dy, dz)
    for dy, dz in ORDER:
        gather.from_core(dy, dz)
    gather.finish()
    load_v.wait()


def prepare(q, table, counts, cache):
    vmem = pl.BlockSpec(memory_space=VMEM)
    hbm = pl.BlockSpec(memory_space=pltpu.HBM)
    return pl.pallas_call(
        prepare_kernel,
        out_shape=(
            jax.ShapeDtypeStruct((Y, Z, C, TILE, HD), BF16),
            jax.ShapeDtypeStruct((BLOCKS, 128), jnp.int32),
            jax.ShapeDtypeStruct((STEPS, 128), jnp.int32),
            jax.ShapeDtypeStruct((PAGES, HD, PAGE), BF16),
            jax.ShapeDtypeStruct((PAGES, PAGE, HD), BF16),
        ),
        in_specs=[hbm, hbm, hbm, hbm],
        out_specs=(vmem,) * 5,
        scratch_shapes=[
            VMEM((SLOTS, BATCH), jnp.int32),
            VMEM((1, BATCH), jnp.int32),
            VMEM((PAGES, PAGE, HD), BF16),
            VMEM((8, BATCH), F32),
            VMEM((STEPS, 128), jnp.int32),
            pltpu.SemaphoreType.DMA((4,)),
            pltpu.SemaphoreType.DMA((2,)),
            *GATHER_SEMS,
        ],
        compiler_params=pltpu.CompilerParams(collective_id=0, has_side_effects=True, vmem_limit_bytes=24 << 20),
        name="prepare",
    )(q, table, counts, cache)


def attend_kernel(pick, who, q_in, kt, v, acc_out, stats_out, q, scores, found):
    def widen(i, carry):
        for j in range(4):
            q[pl.ds((i * 4 + j) * ROWS, ROWS)] = q_in[i * 4 + j].astype(F32).reshape(ROWS, HEADS, HD)
        return carry

    lax.fori_loop(0, BLOCKS // 4, widen, 0)
    found[pl.ds(NONE, 8), 0] = jnp.zeros((8, HEADS, HD), F32)
    found[pl.ds(NONE, 8), 1] = jnp.full((8, HEADS, HD), -1e30, F32)
    ones = jnp.ones((PAGE, HD), BF16)

    def scores_of(g):
        for u in range(UNROLL):
            left = jnp.concatenate([q[who[g, u * CHUNK + j]] for j in range(CHUNK)], axis=0).astype(BF16)
            scores[u] = dot(left, kt[who[g, 64 + u]])

    def weigh(g):
        for u in range(UNROLL):
            at = pl.ds((g * UNROLL + u) * CHUNK, CHUNK)
            s = scores[u] * LOG2E_SCALE
            m = jnp.max(s, axis=1, keepdims=True)
            w = jnp.exp2(s - m).astype(BF16)
            o = dot(w, jnp.concatenate([v[who[g, 64 + u]], ones], axis=1))
            total = o[:, HD:]
            found[at, 0] = (o[:, :HD] / total).reshape(CHUNK, HEADS, HD)
            found[at, 1] = (m + jnp.log2(total)).reshape(CHUNK, HEADS, HD)

    scores_of(0)
    steps = (pick[0, CAP * ROWS] + UNROLL - 1) // UNROLL

    def step(g, carry):
        weigh(g)
        scores_of(jnp.minimum(g + 1, STEPS - 1))
        return carry

    lax.fori_loop(0, steps, step, 0)
    sublane = lax.broadcasted_iota(jnp.int32, (HEADS, HD), 0)
    lane = lax.broadcasted_iota(jnp.int32, (HEADS, HD), 1)

    def close(g, carry):
        tops = jnp.zeros((HEADS, HD), F32)
        totals = jnp.zeros((HEADS, HD), F32)
        outs = []
        for s in range(ROWS):
            at = [pick[g, k * ROWS + s] for k in range(CAP)]
            weights = [found[p, 1] for p in at]
            highest = functools.reduce(jnp.maximum, weights)
            m = jnp.maximum(jnp.floor(highest * 0.5 + 0.5) * 2.0, LOWEST)
            factors = [jnp.exp2(w - m) for w in weights]
            outs.append(sum(f * found[p, 0] for f, p in zip(factors, at)))
            here = lane - sublane == s * HEADS
            tops = jnp.where(here, m, tops)
            totals = jnp.where(here, sum(factors), totals)
        stats_out[g, 0:1] = jnp.sum(tops, axis=0, keepdims=True)
        stats_out[g, 1:2] = jnp.sum(totals, axis=0, keepdims=True)
        acc_out[g] = jnp.concatenate(outs, axis=0).astype(BF16)
        return carry

    lax.fori_loop(0, BLOCKS, close, 0)


def attend(pick, who, q, kt, v):
    vmem = pl.BlockSpec(memory_space=VMEM)
    smem = pl.BlockSpec(memory_space=pltpu.SMEM)
    return pl.pallas_call(
        attend_kernel,
        out_shape=(
            jax.ShapeDtypeStruct((BLOCKS, TILE, HD), BF16),
            jax.ShapeDtypeStruct((BLOCKS, 2, HD), F32),
        ),
        in_specs=[smem, smem, vmem, vmem, vmem],
        out_specs=(vmem, vmem),
        scratch_shapes=[
            VMEM((BATCH, HEADS, HD), F32),
            VMEM((UNROLL, CHUNK * HEADS, PAGE), F32),
            VMEM((NONE + 8, 2, HEADS, HD), F32),
        ],
        compiler_params=pltpu.CompilerParams(vmem_limit_bytes=40 << 20),
        name="attend",
    )(pick, who, q, kt, v)


def merge(parts, stats, diagonal):
    m = functools.reduce(jnp.maximum, [s[0:1] for s in stats])
    factors = [jnp.exp2(s[0:1] - m) for s in stats]
    total = sum(s[1:2] * f for s, f in zip(stats, factors))
    left = jnp.concatenate([jnp.where(diagonal, jnp.broadcast_to(f, (TILE, TILE)), 0.0).astype(BF16) for f in factors], axis=1)
    return dot(left, jnp.concatenate(parts, axis=0)), m, total


def finish_kernel(
    acc, stats, w_ref, out_ref,
    core_acc, core_stats, y_out, y_out_stats, y_in, y_in_stats, z_out, z_out_stats, z_in, z_in_stats,
    turned, att, w, part, parts_in, w_sem,
    c_send, c_recv, cs_send, cs_recv, y_send, y_recv, ys_send, ys_recv, z_send, z_recv, zs_send, zs_recv, h_send, h_recv, *sems,
):
    y, z, c = position()
    h = lax.axis_index("head")
    other = 1 - c
    load_w = pltpu.make_async_copy(w_ref, w, w_sem)
    load_w.start()
    greet(seq_peers(y, z, c) + [{"head": (h + d) % GROUPS} for d in range(1, GROUPS)])
    copies = []
    partner = at_seq(y, z, other)
    order = (2, 1, 3, 0)
    for e in order:
        zz = (z + e) % Z
        copies.append(send(acc.at[:, zz, other], core_acc.at[e], c_send.at[e], c_recv.at[e], partner))
        copies.append(send(stats.at[:, zz, other], core_stats.at[e], cs_send.at[e], cs_recv.at[e], partner))
    diagonal = lax.broadcasted_iota(jnp.int32, (TILE, TILE), 0) == lax.broadcasted_iota(jnp.int32, (TILE, TILE), 1)

    def put(values, rows, o, m, total):
        values[...] = o.astype(BF16)
        rows[0:1] = m
        rows[1:2] = total

    for e in order:
        zz = (z + e) % Z
        arrived(core_acc.at[e], c_send.at[e], c_recv.at[e], partner)
        arrived(core_stats.at[e], cs_send.at[e], cs_recv.at[e], partner)
        for d in order:
            yy = (y + d) % Y
            merged = merge([acc[yy, zz, c], core_acc[e, yy]], [stats[yy, zz, c], core_stats[e, yy]], diagonal)
            if d == 0:
                put(y_in.at[0, e], y_in_stats.at[0, e], *merged)
            else:
                put(y_out.at[d, e], y_out_stats.at[d, e], *merged)
                there = at_seq(yy, z, c)
                copies.append(send(y_out.at[d, e], y_in.at[d, e], y_send.at[d, e], y_recv.at[d, e], there))
                copies.append(send(y_out_stats.at[d, e], y_in_stats.at[d, e], ys_send.at[d, e], ys_recv.at[d, e], there))
    for e in order:
        for d in (1, 3, 2):
            there = at_seq((y - d + Y) % Y, z, c)
            arrived(y_in.at[d, e], y_send.at[d, e], y_recv.at[d, e], there)
            arrived(y_in_stats.at[d, e], ys_send.at[d, e], ys_recv.at[d, e], there)
        merged = merge([y_in[d, e] for d in range(Y)], [y_in_stats[d, e] for d in range(Y)], diagonal)
        if e == 0:
            put(z_in.at[0], z_in_stats.at[0], *merged)
        else:
            put(z_out.at[e], z_out_stats.at[e], *merged)
            there = at_seq(y, (z + e) % Z, c)
            copies.append(send(z_out.at[e], z_in.at[e], z_send.at[e], z_recv.at[e], there))
            copies.append(send(z_out_stats.at[e], z_in_stats.at[e], zs_send.at[e], zs_recv.at[e], there))
    for e in (2, 1, 3):
        there = at_seq(y, (z - e + Z) % Z, c)
        arrived(z_in.at[e], z_send.at[e], z_recv.at[e], there)
        arrived(z_in_stats.at[e], zs_send.at[e], zs_recv.at[e], there)
    o, m, total = merge([z_in[e] for e in range(Z)], [z_in_stats[e] for e in range(Z)], diagonal)
    turned[...] = o / jnp.broadcast_to(total, (TILE, TILE)).T
    for i in range(HEADS):
        att[y, z, c, :, i * HD : (i + 1) * HD] = turned[pl.ds(i, ROWS, stride=HEADS), :].astype(BF16)
    gather = Gather(att, *sems)
    gather.start()
    near = 3 - 2 * (z % 2)
    far = Z - near
    gather.from_z(near)
    gather.from_z(far)
    gather.from_y(1, 0)
    gather.from_y(3, 0)
    gather.from_z(2)
    gather.from_y(2, 0)
    for dy in (1, 3, 2):
        gather.from_y(dy, near)
    load_w.wait()

    def project(pair):
        for yy in range(Y):
            to = yy * 2 + pair
            rows = jnp.concatenate([att[yy, pair * 2 + i, j] for i in range(2) for j in range(C)], axis=0)
            share = dot(rows, w[...]).astype(BF16)

            @pl.when(to == h)
            def _():
                parts_in[h] = share

            @pl.when(to != h)
            def _():
                part[to] = share
                send(part.at[to], parts_in.at[h], h_send.at[to], h_recv.at[h], {"head": to})

    for dz in (0, near):
        for dy in (0, 1, 3, 2):
            gather.from_core(dy, dz)
    project(z // 2)
    for dz in (far, 2):
        for dy in (1, 3, 2):
            gather.from_y(dy, dz)
    for dz in (far, 2):
        for dy in (0, 1, 3, 2):
            gather.from_core(dy, dz)
    project(1 - z // 2)
    for s in range(GROUPS):

        @pl.when(s != h)
        def _():
            arrived(parts_in.at[s], h_send.at[s], h_recv.at[s], {"head": s})

    out_ref[...] = sum(parts_in[s].astype(F32) for s in range(GROUPS)).astype(BF16)
    for s in range(GROUPS):

        @pl.when(s != h)
        def _():
            pltpu.make_async_remote_copy(
                src_ref=part.at[s], dst_ref=parts_in.at[h], send_sem=h_send.at[s], recv_sem=h_recv.at[h],
                device_id={"head": s}, device_id_type=pl.DeviceIdType.MESH,
            ).wait_send()

    gather.finish()
    for copy in copies:
        copy.wait_send()


def finish(acc, stats, w):
    vmem = pl.BlockSpec(memory_space=VMEM)
    width = w.shape[1]
    rows = BATCH // GROUPS
    dma = pltpu.SemaphoreType.DMA
    return pl.pallas_call(
        finish_kernel,
        out_shape=jax.ShapeDtypeStruct((rows, width), BF16),
        in_specs=[vmem, vmem, pl.BlockSpec(memory_space=pltpu.HBM)],
        out_specs=vmem,
        scratch_shapes=[
            VMEM((Z, Y, TILE, HD), BF16), VMEM((Z, Y, 2, HD), F32),
            VMEM((Y, Z, TILE, HD), BF16), VMEM((Y, Z, 2, HD), F32),
            VMEM((Y, Z, TILE, HD), BF16), VMEM((Y, Z, 2, HD), F32),
            VMEM((Z, TILE, HD), BF16), VMEM((Z, 2, HD), F32),
            VMEM((Z, TILE, HD), BF16), VMEM((Z, 2, HD), F32),
            VMEM((TILE, HD), F32),
            VMEM((Y, Z, C, ROWS, HEADS * HD), BF16),
            VMEM((HEADS * HD, width), BF16),
            VMEM((GROUPS, rows, width), BF16), VMEM((GROUPS, rows, width), BF16),
            dma,
            *[dma((Z,)) for _ in range(4)],
            *[dma((Y, Z)) for _ in range(4)],
            *[dma((Z,)) for _ in range(4)],
            dma((GROUPS,)), dma((GROUPS,)),
            *GATHER_SEMS,
        ],
        compiler_params=pltpu.CompilerParams(collective_id=1, has_side_effects=True, vmem_limit_bytes=32 << 20),
        name="finish",
    )(acc, stats, w)


def shards(queries, cache, page_table, page_count, out_weight):
    cache = cache.reshape(2, PAGES, PAGE, HD)
    stay = functools.partial(pltpu.with_memory_space_constraint, memory_space=pltpu.HBM)
    q, pick, who, kt, v = prepare(stay(queries.reshape(TILE, HD)), stay(page_table.T), stay(page_count.reshape(1, BATCH)), stay(cache))
    acc, stats = attend(pick, who, q.reshape(BLOCKS, TILE, HD), kt, v)
    return finish(acc.reshape(Y, Z, C, TILE, HD), stats.reshape(Y, Z, C, 2, HD), stay(out_weight))


def solution(mesh):
    return jax.shard_map(
        shards,
        mesh=mesh,
        in_specs=(
            P("seq", "head", None),
            P(None, "seq", "head", None, None),
            P(),
            P(),
            P("head", "seq"),
        ),
        out_specs=P("head", "seq"),
        check_vma=False,
    )
```

```python
import functools
import math

import jax
import jax.numpy as jnp
from jax import lax
from jax.experimental import pallas as pl
from jax.experimental.pallas import tpu as pltpu
from jax.sharding import PartitionSpec as P

Y, Z, C = 4, 4, 2
BLOCKS = Y * Z * C
ROWS = 16
HEADS = 8
HD = 128
PAGE = 128
PAGES = 64
SLOTS = 64
BATCH = BLOCKS * ROWS
TILE = ROWS * HEADS
GROUPS = 8
CAP = 4
CHUNK = 8
UNROLL = 8
NONE = 2560
STEPS = NONE // CHUNK // UNROLL
LOWEST = -1000.0
LOG2E_SCALE = math.log2(math.e) / math.sqrt(HD)
F32, BF16 = jnp.float32, jnp.bfloat16
VMEM = pltpu.VMEM


def position():
    me = lax.axis_index("seq")
    return me // (Z * C), (me // C) % Z, me % C


def at_seq(y, z, c):
    return {"seq": (y * Z + z) * C + c}


def send(src, dst, send_sem, recv_sem, device):
    copy = pltpu.make_async_remote_copy(
        src_ref=src, dst_ref=dst, send_sem=send_sem, recv_sem=recv_sem,
        device_id=device, device_id_type=pl.DeviceIdType.MESH,
    )
    copy.start()
    return copy


def arrived(dst, send_sem, recv_sem, device):
    pltpu.make_async_remote_copy(
        src_ref=dst, dst_ref=dst, send_sem=send_sem, recv_sem=recv_sem,
        device_id=device, device_id_type=pl.DeviceIdType.MESH,
    ).wait_recv()


def seq_peers(y, z, c):
    peers = [at_seq(y, z, 1 - c)]
    peers += [at_seq(y, (z + d) % Z, c) for d in range(1, Z)]
    peers += [at_seq((y + d) % Y, z, c) for d in range(1, Y)]
    return peers


def greet(peers, meanwhile=None):
    barrier = pltpu.get_barrier_semaphore()
    for peer in peers:
        pl.semaphore_signal(barrier, inc=1, device_id=peer, device_id_type=pl.DeviceIdType.MESH)
    if meanwhile is not None:
        meanwhile()
    pl.semaphore_wait(barrier, len(peers))


class Gather:
    def __init__(self, buf, zs, zr, ys, yr, ds, dr):
        self.buf, self.sems = buf, (zs, zr, ys, yr, ds, dr)
        self.y, self.z, self.c = position()
        self.copies = []

    def spread(self, dz):
        y, z, c = self.y, self.z, self.c
        zs, zr, ys, yr, ds, dr = self.sems
        block = self.buf.at[y, (z - dz + Z) % Z, c]
        for dy in (2, 1, 3):
            self.copies.append(send(block, block, ys.at[dy, dz], yr.at[dy, dz], at_seq((y + dy) % Y, z, c)))
        self.copies.append(send(block, block, ds.at[0, dz], dr.at[0, dz], at_seq(y, z, 1 - c)))

    def start(self):
        y, z, c = self.y, self.z, self.c
        zs, zr, ys, yr, ds, dr = self.sems
        own = self.buf.at[y, z, c]
        for dz in (2, 1, 3):
            self.copies.append(send(own, own, zs.at[dz], zr.at[dz], at_seq(y, (z + dz) % Z, c)))
        self.spread(0)

    def from_z(self, dz):
        y, z, c = self.y, self.z, self.c
        zs, zr, ys, yr, ds, dr = self.sems
        arrived(self.buf.at[y, (z - dz + Z) % Z, c], zs.at[dz], zr.at[dz], at_seq(y, (z - dz + Z) % Z, c))
        self.spread(dz)

    def from_y(self, dy, dz):
        y, z, c = self.y, self.z, self.c
        zs, zr, ys, yr, ds, dr = self.sems
        block = self.buf.at[(y - dy + Y) % Y, (z - dz + Z) % Z, c]
        arrived(block, ys.at[dy, dz], yr.at[dy, dz], at_seq((y - dy + Y) % Y, z, c))
        self.copies.append(send(block, block, ds.at[dy, dz], dr.at[dy, dz], at_seq(y, z, 1 - c)))

    def from_core(self, dy, dz):
        y, z, c = self.y, self.z, self.c
        zs, zr, ys, yr, ds, dr = self.sems
        block = self.buf.at[(y - dy + Y) % Y, (z - dz + Z) % Z, 1 - c]
        arrived(block, ds.at[dy, dz], dr.at[dy, dz], at_seq(y, z, 1 - c))

    def finish(self):
        for copy in self.copies:
            copy.wait_send()


ORDER = [(0, 0)] + [(0, d) for d in (1, 3, 2)] + [(dy, dz) for dz in (0, 1, 3, 2) for dy in (1, 3, 2)]
GATHER_SEMS = [
    pltpu.SemaphoreType.DMA((Z,)), pltpu.SemaphoreType.DMA((Z,)),
    pltpu.SemaphoreType.DMA((Y, Z)), pltpu.SemaphoreType.DMA((Y, Z)),
    pltpu.SemaphoreType.DMA((Y, Z)), pltpu.SemaphoreType.DMA((Y, Z)),
]


def dot(a, b, dims=((1,), (0,))):
    return lax.dot_general(a, b, (dims, ((), ())), preferred_element_type=F32)


def square(n, f):
    return f(lax.broadcasted_iota(jnp.int32, (n, n), 0), lax.broadcasted_iota(jnp.int32, (n, n), 1)).astype(F32).astype(BF16)


def selection(table, counts):
    own = lax.axis_index("seq")
    page = (table % PAGES).astype(F32)
    slot = lax.broadcasted_iota(jnp.int32, (SLOTS, BATCH), 0)
    present = (slot < counts) & (table // PAGES == own)
    rank = dot(square(SLOTS, jnp.greater_equal), present.astype(F32).astype(BF16))
    picks = [jnp.sum(jnp.where(present & (rank == k + 1.0), page + 1.0, 0.0), axis=0, keepdims=True) for k in range(CAP)]
    number = lax.broadcasted_iota(jnp.int32, (PAGES, BATCH), 0).astype(F32)
    takes = [number + 1.0 == pick for pick in picks]
    taken = sum(take.astype(F32) for take in takes)
    before = dot(taken.astype(BF16), square(BATCH, jnp.less_equal))
    chunks = jnp.floor((jnp.sum(taken, axis=1, keepdims=True) + (CHUNK - 1.0)) * (1.0 / CHUNK))
    first = dot(square(PAGES, jnp.greater), jnp.broadcast_to(chunks, (PAGES, 128)).astype(BF16))[:, 0:1]
    place = first * CHUNK + before - 1.0
    places = [
        jnp.where(pick > 0.0, jnp.sum(jnp.where(take, place, 0.0), axis=0, keepdims=True), float(NONE))
        for pick, take in zip(picks, takes)
    ]
    total = jnp.sum(chunks, axis=0, keepdims=True)
    group = lax.broadcasted_iota(jnp.int32, (BLOCKS, BATCH), 0)
    mine = group == lax.broadcasted_iota(jnp.int32, (BLOCKS, BATCH), 1) // ROWS
    column = lax.broadcasted_iota(jnp.int32, (BATCH, 128), 1)
    within = lax.broadcasted_iota(jnp.int32, (BATCH, 128), 0) % ROWS
    high = jnp.zeros((BLOCKS, 128), F32)
    low = jnp.zeros((BLOCKS, 128), F32)
    for k, p in enumerate(places):
        put = (column == k * ROWS + within).astype(F32).astype(BF16)
        upper = jnp.floor(p * (1.0 / 16.0))
        high += dot(jnp.where(mine, upper, 0.0).astype(BF16), put)
        low += dot(jnp.where(mine, p - upper * 16.0, 0.0).astype(BF16), put)
    lane = lax.broadcasted_iota(jnp.int32, (BLOCKS, 128), 1)
    pick = jnp.where(lane == CAP * ROWS, total, high * 16.0 + low)
    chunk = lax.broadcasted_iota(jnp.int32, (PAGES, BATCH), 1).astype(F32)
    page_of = jnp.sum(jnp.where((first <= chunk) & (chunk < first + chunks), number, 0.0), axis=0, keepdims=True)
    step = lax.broadcasted_iota(jnp.int32, (STEPS, BATCH), 0)
    its = step == lax.broadcasted_iota(jnp.int32, (STEPS, BATCH), 1) // UNROLL
    put = (column == 64 + lax.broadcasted_iota(jnp.int32, (BATCH, 128), 0) % UNROLL).astype(F32).astype(BF16)
    pages = dot(jnp.where(its, page_of, 0.0).astype(BF16), put)
    return places, pick.astype(jnp.int32), pages.astype(jnp.int32)


def owners(places, start):
    at = lax.broadcasted_iota(jnp.int32, (256, BATCH), 0).astype(F32) + start.astype(F32)
    hit = (at == places[0:1]) | (at == places[1:2]) | (at == places[2:3]) | (at == places[3:4])
    who = lax.broadcasted_iota(jnp.int32, (8, BATCH), 1)
    digit = jnp.where(lax.broadcasted_iota(jnp.int32, (8, BATCH), 0) == 0, who // 16, who % 16)
    digits = dot(digit.astype(F32).astype(BF16), jnp.where(hit, 1.0, 0.0).astype(BF16), ((1,), (1,)))
    return (digits[0:1] * 16.0 + digits[1:2]).astype(jnp.int32)


def prepare_kernel(
    q_ref, table_ref, counts_ref, cache_ref, all_ref, pick_ref, who_ref, kt_ref, v_ref,
    table, counts, keys, places, pages, in_sems, key_sems, *sems,
):
    y, z, c = position()
    half = PAGES // 2
    small = [
        pltpu.make_async_copy(q_ref, all_ref.at[y, z, c], in_sems.at[0]),
        pltpu.make_async_copy(table_ref, table, in_sems.at[1]),
        pltpu.make_async_copy(counts_ref, counts, in_sems.at[2]),
    ]
    loads = [
        pltpu.make_async_copy(cache_ref.at[0, pl.ds(i * half, half)], keys.at[pl.ds(i * half, half)], key_sems.at[i])
        for i in range(2)
    ]
    load_v = pltpu.make_async_copy(cache_ref.at[1], v_ref, in_sems.at[3])
    for load in small + loads:
        load.start()
    greet(seq_peers(y, z, c))
    small[0].wait()
    gather = Gather(all_ref, *sems)
    gather.start()
    load_v.start()
    small[1].wait()
    small[2].wait()
    rows, pick_ref[...], pages[...] = selection(table[...], counts[...])
    for k in range(CAP):
        places[k : k + 1] = rows[k]

    def turn(i, carry):
        for j in range(4):
            kt_ref[i * 4 + j] = keys[i * 4 + j].T
        return carry

    def name(i, carry):
        lane = lax.broadcasted_iota(jnp.int32, (1, 128), 1)
        who = owners(places, i * 256)
        for j in range(2):
            half_row = who[:, j * 128 : (j + 1) * 128]
            rolled = pltpu.roll(jnp.broadcast_to(half_row, (8, 128)), 64, 1)[0:1]
            row = 4 * i + 2 * j
            who_ref[pl.ds(row, 1)] = jnp.where(lane < 64, half_row, pages[pl.ds(row, 1)])
            who_ref[pl.ds(row + 1, 1)] = jnp.where(lane < 64, rolled, pages[pl.ds(row + 1, 1)])
        return carry

    loads[0].wait()
    lax.fori_loop(0, 8, turn, 0)
    for dz in (1, 3, 2):
        gather.from_z(dz)
    loads[1].wait()
    lax.fori_loop(8, 16, turn, 0)
    lax.fori_loop(0, NONE // 256, name, 0)
    for dy, dz in ORDER[4:]:
        gather.from_y(dy, dz)
    for dy, dz in ORDER:
        gather.from_core(dy, dz)
    gather.finish()
    load_v.wait()


def prepare(q, table, counts, cache):
    vmem = pl.BlockSpec(memory_space=VMEM)
    hbm = pl.BlockSpec(memory_space=pltpu.HBM)
    return pl.pallas_call(
        prepare_kernel,
        out_shape=(
            jax.ShapeDtypeStruct((Y, Z, C, TILE, HD), BF16),
            jax.ShapeDtypeStruct((BLOCKS, 128), jnp.int32),
            jax.ShapeDtypeStruct((STEPS, 128), jnp.int32),
            jax.ShapeDtypeStruct((PAGES, HD, PAGE), BF16),
            jax.ShapeDtypeStruct((PAGES, PAGE, HD), BF16),
        ),
        in_specs=[hbm, hbm, hbm, hbm],
        out_specs=(vmem,) * 5,
        scratch_shapes=[
            VMEM((SLOTS, BATCH), jnp.int32),
            VMEM((1, BATCH), jnp.int32),
            VMEM((PAGES, PAGE, HD), BF16),
            VMEM((8, BATCH), F32),
            VMEM((STEPS, 128), jnp.int32),
            pltpu.SemaphoreType.DMA((4,)),
            pltpu.SemaphoreType.DMA((2,)),
            *GATHER_SEMS,
        ],
        compiler_params=pltpu.CompilerParams(collective_id=0, has_side_effects=True, vmem_limit_bytes=12 << 20),
        name="prepare",
    )(q, table, counts, cache)


def attend_kernel(pick, who, q_in, kt, v, found, q, scores):
    def widen(i, carry):
        for j in range(4):
            q[pl.ds((i * 4 + j) * ROWS, ROWS)] = q_in[i * 4 + j].astype(F32).reshape(ROWS, HEADS, HD)
        return carry

    lax.fori_loop(0, BLOCKS // 4, widen, 0)
    found[pl.ds(NONE, 8), 0] = jnp.zeros((8, HEADS, HD), F32)
    found[pl.ds(NONE, 8), 1] = jnp.full((8, HEADS, HD), -1e30, F32)
    ones = jnp.ones((PAGE, HD), BF16)

    def scores_of(g):
        for u in range(UNROLL):
            left = jnp.concatenate([q[who[g, u * CHUNK + j]] for j in range(CHUNK)], axis=0).astype(BF16)
            scores[u] = dot(left, kt[who[g, 64 + u]])

    def weigh(g):
        for u in range(UNROLL):
            at = pl.ds((g * UNROLL + u) * CHUNK, CHUNK)
            s = scores[u] * LOG2E_SCALE
            m = jnp.max(s, axis=1, keepdims=True)
            w = jnp.exp2(s - m).astype(BF16)
            o = dot(w, jnp.concatenate([v[who[g, 64 + u]], ones], axis=1))
            total = o[:, HD:]
            found[at, 0] = (o[:, :HD] / total).reshape(CHUNK, HEADS, HD)
            found[at, 1] = (m + jnp.log2(total)).reshape(CHUNK, HEADS, HD)

    scores_of(0)
    steps = (pick[0, CAP * ROWS] + UNROLL - 1) // UNROLL

    def step(g, carry):
        weigh(g)
        scores_of(jnp.minimum(g + 1, STEPS - 1))
        return carry

    lax.fori_loop(0, steps, step, 0)


def attend(pick, who, q, kt, v):
    vmem = pl.BlockSpec(memory_space=VMEM)
    smem = pl.BlockSpec(memory_space=pltpu.SMEM)
    return pl.pallas_call(
        attend_kernel,
        out_shape=VMEM((NONE + 8, 2, HEADS, HD), F32),
        in_specs=[smem, smem, vmem, vmem, vmem],
        out_specs=vmem,
        scratch_shapes=[
            VMEM((BATCH, HEADS, HD), F32),
            VMEM((UNROLL, CHUNK * HEADS, PAGE), F32),
        ],
        compiler_params=pltpu.CompilerParams(vmem_limit_bytes=8 << 20),
        name="attend",
    )(pick, who, q, kt, v)


def settle(pick, found, g, values, stats):
    sublane = lax.broadcasted_iota(jnp.int32, (HEADS, HD), 0)
    lane = lax.broadcasted_iota(jnp.int32, (HEADS, HD), 1)
    tops = jnp.zeros((HEADS, HD), F32)
    totals = jnp.zeros((HEADS, HD), F32)
    outs = []
    for s in range(ROWS):
        at = [pick[g, k * ROWS + s] for k in range(CAP)]
        highest = [found[p, 1] for p in at]
        m = jnp.maximum(jnp.floor(functools.reduce(jnp.maximum, highest) * 0.5 + 0.5) * 2.0, LOWEST)
        factors = [jnp.exp2(t - m) for t in highest]
        outs.append(sum(f * found[p, 0] for f, p in zip(factors, at)))
        here = lane - sublane == s * HEADS
        tops = jnp.where(here, m, tops)
        totals = jnp.where(here, sum(factors), totals)
    stats[0:1] = jnp.sum(tops, axis=0, keepdims=True)
    stats[1:2] = jnp.sum(totals, axis=0, keepdims=True)
    values[...] = jnp.concatenate(outs, axis=0).astype(BF16)


def merge(parts, stats, diagonal):
    m = functools.reduce(jnp.maximum, [s[0:1] for s in stats])
    factors = [jnp.exp2(s[0:1] - m) for s in stats]
    total = sum(s[1:2] * f for s, f in zip(stats, factors))
    left = jnp.concatenate([jnp.where(diagonal, jnp.broadcast_to(f, (TILE, TILE)), 0.0).astype(BF16) for f in factors], axis=1)
    return dot(left, jnp.concatenate(parts, axis=0)), m, total


def finish_kernel(
    pick, found, w_ref, out_ref,
    own_acc, own_stats, their_acc, their_stats,
    core_acc, core_stats, y_out, y_out_stats, y_in, y_in_stats, z_out, z_out_stats, z_in, z_in_stats,
    turned, att, w, part, parts_in, w_sem,
    c_send, c_recv, cs_send, cs_recv, y_send, y_recv, ys_send, ys_recv, z_send, z_recv, zs_send, zs_recv, h_send, h_recv, *sems,
):
    y, z, c = position()
    h = lax.axis_index("head")
    other = 1 - c
    load_w = pltpu.make_async_copy(w_ref, w, w_sem)
    load_w.start()
    partner = at_seq(y, z, other)
    order = (2, 1, 3, 0)

    def settle_all(e, core, values, stats):
        def one(yy, carry):
            settle(pick, found, (yy * Z + (z + e) % Z) * C + core, values.at[e, yy], stats.at[e, yy])
            return carry

        lax.fori_loop(0, Y, one, 0)

    def theirs():
        for e in order:
            settle_all(e, other, their_acc, their_stats)

    greet(seq_peers(y, z, c) + [{"head": (h + d) % GROUPS} for d in range(1, GROUPS)], theirs)
    copies = []
    for e in order:
        copies.append(send(their_acc.at[e], core_acc.at[e], c_send.at[e], c_recv.at[e], partner))
        copies.append(send(their_stats.at[e], core_stats.at[e], cs_send.at[e], cs_recv.at[e], partner))
    diagonal = lax.broadcasted_iota(jnp.int32, (TILE, TILE), 0) == lax.broadcasted_iota(jnp.int32, (TILE, TILE), 1)

    def put(values, rows, o, m, total):
        values[...] = o.astype(BF16)
        rows[0:1] = m
        rows[1:2] = total

    for e in order:
        settle_all(e, c, own_acc, own_stats)
        arrived(core_acc.at[e], c_send.at[e], c_recv.at[e], partner)
        arrived(core_stats.at[e], cs_send.at[e], cs_recv.at[e], partner)
        for d in order:
            yy = (y + d) % Y
            merged = merge([own_acc[e, yy], core_acc[e, yy]], [own_stats[e, yy], core_stats[e, yy]], diagonal)
            if d == 0:
                put(y_in.at[0, e], y_in_stats.at[0, e], *merged)
            else:
                put(y_out.at[d, e], y_out_stats.at[d, e], *merged)
                there = at_seq(yy, z, c)
                copies.append(send(y_out.at[d, e], y_in.at[d, e], y_send.at[d, e], y_recv.at[d, e], there))
                copies.append(send(y_out_stats.at[d, e], y_in_stats.at[d, e], ys_send.at[d, e], ys_recv.at[d, e], there))
    for e in order:
        for d in (1, 3, 2):
            there = at_seq((y - d + Y) % Y, z, c)
            arrived(y_in.at[d, e], y_send.at[d, e], y_recv.at[d, e], there)
            arrived(y_in_stats.at[d, e], ys_send.at[d, e], ys_recv.at[d, e], there)
        merged = merge([y_in[d, e] for d in range(Y)], [y_in_stats[d, e] for d in range(Y)], diagonal)
        if e == 0:
            put(z_in.at[0], z_in_stats.at[0], *merged)
        else:
            put(z_out.at[e], z_out_stats.at[e], *merged)
            there = at_seq(y, (z + e) % Z, c)
            copies.append(send(z_out.at[e], z_in.at[e], z_send.at[e], z_recv.at[e], there))
            copies.append(send(z_out_stats.at[e], z_in_stats.at[e], zs_send.at[e], zs_recv.at[e], there))
    for e in (2, 1, 3):
        there = at_seq(y, (z - e + Z) % Z, c)
        arrived(z_in.at[e], z_send.at[e], z_recv.at[e], there)
        arrived(z_in_stats.at[e], zs_send.at[e], zs_recv.at[e], there)
    o, m, total = merge([z_in[e] for e in range(Z)], [z_in_stats[e] for e in range(Z)], diagonal)
    turned[...] = o / jnp.broadcast_to(total, (TILE, TILE)).T
    for i in range(HEADS):
        att[y, z, c, :, i * HD : (i + 1) * HD] = turned[pl.ds(i, ROWS, stride=HEADS), :].astype(BF16)
    gather = Gather(att, *sems)
    gather.start()
    near = 3 - 2 * (z % 2)
    far = Z - near
    gather.from_z(near)
    gather.from_z(far)
    gather.from_y(1, 0)
    gather.from_y(3, 0)
    gather.from_z(2)
    gather.from_y(2, 0)
    for dy in (1, 3, 2):
        gather.from_y(dy, near)
    load_w.wait()

    def project(pair):
        for yy in range(Y):
            to = yy * 2 + pair
            rows = jnp.concatenate([att[yy, pair * 2 + i, j] for i in range(2) for j in range(C)], axis=0)
            share = dot(rows, w[...]).astype(BF16)

            @pl.when(to == h)
            def _():
                parts_in[h] = share

            @pl.when(to != h)
            def _():
                part[to] = share
                send(part.at[to], parts_in.at[h], h_send.at[to], h_recv.at[h], {"head": to})

    for dz in (0, near):
        for dy in (0, 1, 3, 2):
            gather.from_core(dy, dz)
    project(z // 2)
    for dz in (far, 2):
        for dy in (1, 3, 2):
            gather.from_y(dy, dz)
    for dz in (far, 2):
        for dy in (0, 1, 3, 2):
            gather.from_core(dy, dz)
    project(1 - z // 2)
    for s in range(GROUPS):

        @pl.when(s != h)
        def _():
            arrived(parts_in.at[s], h_send.at[s], h_recv.at[s], {"head": s})

    out_ref[...] = sum(parts_in[s].astype(F32) for s in range(GROUPS)).astype(BF16)
    for s in range(GROUPS):

        @pl.when(s != h)
        def _():
            pltpu.make_async_remote_copy(
                src_ref=part.at[s], dst_ref=parts_in.at[h], send_sem=h_send.at[s], recv_sem=h_recv.at[h],
                device_id={"head": s}, device_id_type=pl.DeviceIdType.MESH,
            ).wait_send()

    gather.finish()
    for copy in copies:
        copy.wait_send()


def finish(pick, found, w):
    vmem = pl.BlockSpec(memory_space=VMEM)
    width = w.shape[1]
    rows = BATCH // GROUPS
    dma = pltpu.SemaphoreType.DMA
    return pl.pallas_call(
        finish_kernel,
        out_shape=jax.ShapeDtypeStruct((rows, width), BF16),
        in_specs=[pl.BlockSpec(memory_space=pltpu.SMEM), vmem, pl.BlockSpec(memory_space=pltpu.HBM)],
        out_specs=vmem,
        scratch_shapes=[
            VMEM((Z, Y, TILE, HD), BF16), VMEM((Z, Y, 2, HD), F32),
            VMEM((Z, Y, TILE, HD), BF16), VMEM((Z, Y, 2, HD), F32),
            VMEM((Z, Y, TILE, HD), BF16), VMEM((Z, Y, 2, HD), F32),
            VMEM((Y, Z, TILE, HD), BF16), VMEM((Y, Z, 2, HD), F32),
            VMEM((Y, Z, TILE, HD), BF16), VMEM((Y, Z, 2, HD), F32),
            VMEM((Z, TILE, HD), BF16), VMEM((Z, 2, HD), F32),
            VMEM((Z, TILE, HD), BF16), VMEM((Z, 2, HD), F32),
            VMEM((TILE, HD), F32),
            VMEM((Y, Z, C, ROWS, HEADS * HD), BF16),
            VMEM((HEADS * HD, width), BF16),
            VMEM((GROUPS, rows, width), BF16), VMEM((GROUPS, rows, width), BF16),
            dma,
            *[dma((Z,)) for _ in range(4)],
            *[dma((Y, Z)) for _ in range(4)],
            *[dma((Z,)) for _ in range(4)],
            dma((GROUPS,)), dma((GROUPS,)),
            *GATHER_SEMS,
        ],
        compiler_params=pltpu.CompilerParams(collective_id=1, has_side_effects=True, vmem_limit_bytes=12 << 20),
        name="finish",
    )(pick, found, w)


def shards(queries, cache, page_table, page_count, out_weight):
    cache = cache.reshape(2, PAGES, PAGE, HD)
    stay = functools.partial(pltpu.with_memory_space_constraint, memory_space=pltpu.HBM)
    q, pick, who, kt, v = prepare(stay(queries.reshape(TILE, HD)), stay(page_table.T), stay(page_count.reshape(1, BATCH)), stay(cache))
    found = attend(pick, who, q.reshape(BLOCKS, TILE, HD), kt, v)
    return finish(pick, found, stay(out_weight))


def solution(mesh):
    return jax.shard_map(
        shards,
        mesh=mesh,
        in_specs=(
            P("seq", "head", None),
            P(None, "seq", "head", None, None),
            P(),
            P(),
            P("head", "seq"),
        ),
        out_specs=P("head", "seq"),
        check_vma=False,
    )
```

```python
import functools
import math

import jax
import jax.numpy as jnp
from jax import lax
from jax.experimental import pallas as pl
from jax.experimental.pallas import tpu as pltpu
from jax.sharding import PartitionSpec as P

Y, Z, C = 4, 4, 2
BLOCKS = Y * Z * C
ROWS = 16
HEADS = 8
HD = 128
PAGE = 128
PAGES = 64
SLOTS = 64
BATCH = BLOCKS * ROWS
TILE = ROWS * HEADS
GROUPS = 8
CAP = 4
CHUNK = 8
UNROLL = 8
NONE = 2560
STEPS = NONE // CHUNK // UNROLL
LOWEST = -1000.0
LOG2E_SCALE = math.log2(math.e) / math.sqrt(HD)
F32, BF16 = jnp.float32, jnp.bfloat16
VMEM = pltpu.VMEM


def position():
    me = lax.axis_index("seq")
    return me // (Z * C), (me // C) % Z, me % C


def at_seq(y, z, c):
    return {"seq": (y * Z + z) * C + c}


def send(src, dst, send_sem, recv_sem, device):
    copy = pltpu.make_async_remote_copy(
        src_ref=src, dst_ref=dst, send_sem=send_sem, recv_sem=recv_sem,
        device_id=device, device_id_type=pl.DeviceIdType.MESH,
    )
    copy.start()
    return copy


def arrived(dst, send_sem, recv_sem, device):
    pltpu.make_async_remote_copy(
        src_ref=dst, dst_ref=dst, send_sem=send_sem, recv_sem=recv_sem,
        device_id=device, device_id_type=pl.DeviceIdType.MESH,
    ).wait_recv()


def seq_peers(y, z, c):
    peers = [at_seq(y, z, 1 - c)]
    peers += [at_seq(y, (z + d) % Z, c) for d in range(1, Z)]
    peers += [at_seq((y + d) % Y, z, c) for d in range(1, Y)]
    return peers


def greet(peers, meanwhile=None):
    barrier = pltpu.get_barrier_semaphore()
    for peer in peers:
        pl.semaphore_signal(barrier, inc=1, device_id=peer, device_id_type=pl.DeviceIdType.MESH)
    if meanwhile is not None:
        meanwhile()
    pl.semaphore_wait(barrier, len(peers))


class Gather:
    def __init__(self, buf, zs, zr, ys, yr, ds, dr):
        self.buf, self.sems = buf, (zs, zr, ys, yr, ds, dr)
        self.y, self.z, self.c = position()
        self.copies = []

    def block(self, dy, dz, other=False):
        y, z = (self.y - dy + Y) % Y, (self.z - dz + Z) % Z
        c = 1 - self.c if other else self.c
        return self.buf.at[y, z, c]

    def send(self, block, send_sem, recv_sem, y, z, c):
        self.copies.append(send(block, block, send_sem, recv_sem, at_seq((y + Y) % Y, (z + Z) % Z, c)))

    def to_core(self, dy, dz):
        ds, dr = self.sems[4:]
        self.send(self.block(dy, dz), ds.at[dy, dz], dr.at[dy, dz], self.y, self.z, 1 - self.c)

    def along_y(self, dz):
        ys, yr = self.sems[2:4]
        for dy in (2, 1, 3):
            self.send(self.block(0, dz), ys.at[dy, dz], yr.at[dy, dz], self.y + dy, self.z, self.c)

    def start(self):
        zs, zr = self.sems[:2]
        for dz in (2, 1, 3):
            self.send(self.block(0, 0), zs.at[dz], zr.at[dz], self.y, self.z + dz, self.c)
        self.along_y(0)
        self.to_core(0, 0)

    def from_z(self, dz):
        zs, zr = self.sems[:2]
        arrived(self.block(0, dz), zs.at[dz], zr.at[dz], at_seq(self.y, (self.z - dz + Z) % Z, self.c))
        self.along_y(dz)
        self.to_core(0, dz)

    def from_y(self, dy, dz):
        ys, yr = self.sems[2:4]
        arrived(self.block(dy, dz), ys.at[dy, dz], yr.at[dy, dz], at_seq((self.y - dy + Y) % Y, self.z, self.c))
        self.to_core(dy, dz)

    def from_core(self, dy, dz):
        ds, dr = self.sems[4:]
        arrived(self.block(dy, dz, other=True), ds.at[dy, dz], dr.at[dy, dz], at_seq(self.y, self.z, 1 - self.c))

    def finish(self):
        for copy in self.copies:
            copy.wait_send()


GATHER_SEMS = [
    pltpu.SemaphoreType.DMA((Z,)), pltpu.SemaphoreType.DMA((Z,)),
    pltpu.SemaphoreType.DMA((Y, Z)), pltpu.SemaphoreType.DMA((Y, Z)),
    pltpu.SemaphoreType.DMA((Y, Z)), pltpu.SemaphoreType.DMA((Y, Z)),
]


def dot(a, b, dims=((1,), (0,))):
    return lax.dot_general(a, b, (dims, ((), ())), preferred_element_type=F32)


def square(n, f):
    return f(lax.broadcasted_iota(jnp.int32, (n, n), 0), lax.broadcasted_iota(jnp.int32, (n, n), 1)).astype(F32).astype(BF16)


def selection(table, counts):
    own = lax.axis_index("seq")
    page = (table % PAGES).astype(F32)
    slot = lax.broadcasted_iota(jnp.int32, (SLOTS, BATCH), 0)
    present = (slot < counts) & (table // PAGES == own)
    rank = dot(square(SLOTS, jnp.greater_equal), present.astype(F32).astype(BF16))
    picks = [jnp.sum(jnp.where(present & (rank == k + 1.0), page + 1.0, 0.0), axis=0, keepdims=True) for k in range(CAP)]
    number = lax.broadcasted_iota(jnp.int32, (PAGES, BATCH), 0).astype(F32)
    takes = [number + 1.0 == pick for pick in picks]
    taken = sum(take.astype(F32) for take in takes)
    before = dot(taken.astype(BF16), square(BATCH, jnp.less_equal))
    chunks = jnp.floor((jnp.sum(taken, axis=1, keepdims=True) + (CHUNK - 1.0)) * (1.0 / CHUNK))
    first = dot(square(PAGES, jnp.greater), jnp.broadcast_to(chunks, (PAGES, 128)).astype(BF16))[:, 0:1]
    place = first * CHUNK + before - 1.0
    places = [
        jnp.where(pick > 0.0, jnp.sum(jnp.where(take, place, 0.0), axis=0, keepdims=True), float(NONE))
        for pick, take in zip(picks, takes)
    ]
    total = jnp.sum(chunks, axis=0, keepdims=True)
    group = lax.broadcasted_iota(jnp.int32, (BLOCKS, BATCH), 0)
    mine = group == lax.broadcasted_iota(jnp.int32, (BLOCKS, BATCH), 1) // ROWS
    column = lax.broadcasted_iota(jnp.int32, (BATCH, 128), 1)
    within = lax.broadcasted_iota(jnp.int32, (BATCH, 128), 0) % ROWS
    high = jnp.zeros((BLOCKS, 128), F32)
    low = jnp.zeros((BLOCKS, 128), F32)
    for k, p in enumerate(places):
        put = (column == k * ROWS + within).astype(F32).astype(BF16)
        upper = jnp.floor(p * (1.0 / 16.0))
        high += dot(jnp.where(mine, upper, 0.0).astype(BF16), put)
        low += dot(jnp.where(mine, p - upper * 16.0, 0.0).astype(BF16), put)
    lane = lax.broadcasted_iota(jnp.int32, (BLOCKS, 128), 1)
    pick = jnp.where(lane == CAP * ROWS, total, high * 16.0 + low)
    chunk = lax.broadcasted_iota(jnp.int32, (PAGES, BATCH), 1).astype(F32)
    page_of = jnp.sum(jnp.where((first <= chunk) & (chunk < first + chunks), number, 0.0), axis=0, keepdims=True)
    step = lax.broadcasted_iota(jnp.int32, (STEPS, BATCH), 0)
    its = step == lax.broadcasted_iota(jnp.int32, (STEPS, BATCH), 1) // UNROLL
    put = (column == 64 + lax.broadcasted_iota(jnp.int32, (BATCH, 128), 0) % UNROLL).astype(F32).astype(BF16)
    pages = dot(jnp.where(its, page_of, 0.0).astype(BF16), put)
    return places, pick.astype(jnp.int32), pages.astype(jnp.int32)


def owners(places, start):
    at = lax.broadcasted_iota(jnp.int32, (256, BATCH), 0).astype(F32) + start.astype(F32)
    hit = (at == places[0:1]) | (at == places[1:2]) | (at == places[2:3]) | (at == places[3:4])
    who = lax.broadcasted_iota(jnp.int32, (8, BATCH), 1)
    digit = jnp.where(lax.broadcasted_iota(jnp.int32, (8, BATCH), 0) == 0, who // 16, who % 16)
    digits = dot(digit.astype(F32).astype(BF16), jnp.where(hit, 1.0, 0.0).astype(BF16), ((1,), (1,)))
    return (digits[0:1] * 16.0 + digits[1:2]).astype(jnp.int32)


def prepare_kernel(
    q_ref, table_ref, counts_ref, cache_ref, all_ref, pick_ref, who_ref, kt_ref, v_ref,
    table, counts, keys, places, pages, in_sems, key_sems, *sems,
):
    y, z, c = position()
    half = PAGES // 2
    small = [
        pltpu.make_async_copy(q_ref, all_ref.at[y, z, c], in_sems.at[0]),
        pltpu.make_async_copy(table_ref, table, in_sems.at[1]),
        pltpu.make_async_copy(counts_ref, counts, in_sems.at[2]),
    ]
    loads = [
        pltpu.make_async_copy(cache_ref.at[0, pl.ds(i * half, half)], keys.at[pl.ds(i * half, half)], key_sems.at[i])
        for i in range(2)
    ]
    load_v = pltpu.make_async_copy(cache_ref.at[1], v_ref, in_sems.at[3])
    for load in small + loads:
        load.start()
    greet(seq_peers(y, z, c))
    small[0].wait()
    gather = Gather(all_ref, *sems)
    gather.start()
    load_v.start()
    small[1].wait()
    small[2].wait()
    rows, pick_ref[...], pages[...] = selection(table[...], counts[...])
    for k in range(CAP):
        places[k : k + 1] = rows[k]

    def turn(i, carry):
        for j in range(4):
            kt_ref[i * 4 + j] = keys[i * 4 + j].T
        return carry

    def name(i, carry):
        lane = lax.broadcasted_iota(jnp.int32, (1, 128), 1)
        who = owners(places, i * 256)
        for j in range(2):
            half_row = who[:, j * 128 : (j + 1) * 128]
            rolled = pltpu.roll(jnp.broadcast_to(half_row, (8, 128)), 64, 1)[0:1]
            row = 4 * i + 2 * j
            who_ref[pl.ds(row, 1)] = jnp.where(lane < 64, half_row, pages[pl.ds(row, 1)])
            who_ref[pl.ds(row + 1, 1)] = jnp.where(lane < 64, rolled, pages[pl.ds(row + 1, 1)])
        return carry

    loads[0].wait()
    lax.fori_loop(0, 8, turn, 0)
    for dz in (1, 3, 2):
        gather.from_z(dz)
    loads[1].wait()
    lax.fori_loop(8, 16, turn, 0)
    lax.fori_loop(0, NONE // 256, name, 0)
    for dz in (0, 1, 3, 2):
        for dy in (1, 3, 2):
            gather.from_y(dy, dz)
    for dz in (0, 1, 3, 2):
        for dy in range(Y):
            gather.from_core(dy, dz)
    gather.finish()
    load_v.wait()


def prepare(q, table, counts, cache):
    vmem = pl.BlockSpec(memory_space=VMEM)
    hbm = pl.BlockSpec(memory_space=pltpu.HBM)
    return pl.pallas_call(
        prepare_kernel,
        out_shape=(
            jax.ShapeDtypeStruct((Y, Z, C, TILE, HD), BF16),
            jax.ShapeDtypeStruct((BLOCKS, 128), jnp.int32),
            jax.ShapeDtypeStruct((STEPS, 128), jnp.int32),
            jax.ShapeDtypeStruct((PAGES, HD, PAGE), BF16),
            jax.ShapeDtypeStruct((PAGES, PAGE, HD), BF16),
        ),
        in_specs=[hbm, hbm, hbm, hbm],
        out_specs=(vmem,) * 5,
        scratch_shapes=[
            VMEM((SLOTS, BATCH), jnp.int32),
            VMEM((1, BATCH), jnp.int32),
            VMEM((PAGES, PAGE, HD), BF16),
            VMEM((8, BATCH), F32),
            VMEM((STEPS, 128), jnp.int32),
            pltpu.SemaphoreType.DMA((4,)),
            pltpu.SemaphoreType.DMA((2,)),
            *GATHER_SEMS,
        ],
        compiler_params=pltpu.CompilerParams(collective_id=0, has_side_effects=True, vmem_limit_bytes=12 << 20),
        name="prepare",
    )(q, table, counts, cache)


def attend_kernel(pick, who, q_in, kt, v, found, q, scores):
    def widen(i, carry):
        for j in range(4):
            q[pl.ds((i * 4 + j) * ROWS, ROWS)] = q_in[i * 4 + j].astype(F32).reshape(ROWS, HEADS, HD)
        return carry

    lax.fori_loop(0, BLOCKS // 4, widen, 0)
    found[pl.ds(NONE, 8), 0] = jnp.zeros((8, HEADS, HD), F32)
    found[pl.ds(NONE, 8), 1] = jnp.full((8, HEADS, HD), -1e30, F32)
    ones = jnp.ones((PAGE, HD), BF16)

    def scores_of(g):
        for u in range(UNROLL):
            left = jnp.concatenate([q[who[g, u * CHUNK + j]] for j in range(CHUNK)], axis=0).astype(BF16)
            scores[u] = dot(left, kt[who[g, 64 + u]])

    def weigh(g):
        for u in range(UNROLL):
            at = pl.ds((g * UNROLL + u) * CHUNK, CHUNK)
            s = scores[u] * LOG2E_SCALE
            m = jnp.max(s, axis=1, keepdims=True)
            w = jnp.exp2(s - m).astype(BF16)
            o = dot(w, jnp.concatenate([v[who[g, 64 + u]], ones], axis=1))
            total = o[:, HD:]
            found[at, 0] = (o[:, :HD] / total).reshape(CHUNK, HEADS, HD)
            found[at, 1] = (m + jnp.log2(total)).reshape(CHUNK, HEADS, HD)

    scores_of(0)
    steps = (pick[0, CAP * ROWS] + UNROLL - 1) // UNROLL

    def step(g, carry):
        weigh(g)
        scores_of(jnp.minimum(g + 1, STEPS - 1))
        return carry

    lax.fori_loop(0, steps, step, 0)


def attend(pick, who, q, kt, v):
    vmem = pl.BlockSpec(memory_space=VMEM)
    smem = pl.BlockSpec(memory_space=pltpu.SMEM)
    return pl.pallas_call(
        attend_kernel,
        out_shape=VMEM((NONE + 8, 2, HEADS, HD), F32),
        in_specs=[smem, smem, vmem, vmem, vmem],
        out_specs=vmem,
        scratch_shapes=[
            VMEM((BATCH, HEADS, HD), F32),
            VMEM((UNROLL, CHUNK * HEADS, PAGE), F32),
        ],
        compiler_params=pltpu.CompilerParams(vmem_limit_bytes=8 << 20),
        name="attend",
    )(pick, who, q, kt, v)


def settle(pick, found, g, values, stats):
    sublane = lax.broadcasted_iota(jnp.int32, (HEADS, HD), 0)
    lane = lax.broadcasted_iota(jnp.int32, (HEADS, HD), 1)
    tops = jnp.zeros((HEADS, HD), F32)
    totals = jnp.zeros((HEADS, HD), F32)
    outs = []
    for s in range(ROWS):
        at = [pick[g, k * ROWS + s] for k in range(CAP)]
        highest = [found[p, 1] for p in at]
        m = jnp.maximum(jnp.floor(functools.reduce(jnp.maximum, highest) * 0.5 + 0.5) * 2.0, LOWEST)
        factors = [jnp.exp2(t - m) for t in highest]
        outs.append(sum(f * found[p, 0] for f, p in zip(factors, at)))
        here = lane - sublane == s * HEADS
        tops = jnp.where(here, m, tops)
        totals = jnp.where(here, sum(factors), totals)
    stats[0:1] = jnp.sum(tops, axis=0, keepdims=True)
    stats[1:2] = jnp.sum(totals, axis=0, keepdims=True)
    values[...] = jnp.concatenate(outs, axis=0).astype(BF16)


def merge(parts, stats, diagonal):
    m = functools.reduce(jnp.maximum, [s[0:1] for s in stats])
    factors = [jnp.exp2(s[0:1] - m) for s in stats]
    total = sum(s[1:2] * f for s, f in zip(stats, factors))
    left = jnp.concatenate([jnp.where(diagonal, jnp.broadcast_to(f, (TILE, TILE)), 0.0).astype(BF16) for f in factors], axis=1)
    return dot(left, jnp.concatenate(parts, axis=0)), m, total


def finish_kernel(
    pick, found, w_ref, out_ref,
    own_acc, own_stats, their_acc, their_stats,
    core_acc, core_stats, y_out, y_out_stats, y_in, y_in_stats, z_out, z_out_stats, z_in, z_in_stats,
    turned, att, w, part, parts_in, w_sem,
    c_send, c_recv, cs_send, cs_recv, y_send, y_recv, ys_send, ys_recv, z_send, z_recv, zs_send, zs_recv, h_send, h_recv, *sems,
):
    y, z, c = position()
    h = lax.axis_index("head")
    other = 1 - c
    load_w = pltpu.make_async_copy(w_ref, w, w_sem)
    load_w.start()
    partner = at_seq(y, z, other)
    order = (2, 1, 3, 0)

    def settle_all(e, core, values, stats):
        def one(yy, carry):
            settle(pick, found, (yy * Z + (z + e) % Z) * C + core, values.at[e, yy], stats.at[e, yy])
            return carry

        lax.fori_loop(0, Y, one, 0)

    def early():
        for e in order:
            settle_all(e, other, their_acc, their_stats)
        settle_all(order[0], c, own_acc, own_stats)

    greet(seq_peers(y, z, c) + [{"head": (h + d) % GROUPS} for d in range(1, GROUPS)], early)
    copies = []
    for e in order:
        copies.append(send(their_acc.at[e], core_acc.at[e], c_send.at[e], c_recv.at[e], partner))
        copies.append(send(their_stats.at[e], core_stats.at[e], cs_send.at[e], cs_recv.at[e], partner))
    diagonal = lax.broadcasted_iota(jnp.int32, (TILE, TILE), 0) == lax.broadcasted_iota(jnp.int32, (TILE, TILE), 1)

    def put(values, rows, o, m, total):
        values[...] = o.astype(BF16)
        rows[0:1] = m
        rows[1:2] = total

    for e in order:
        if e != order[0]:
            settle_all(e, c, own_acc, own_stats)
        arrived(core_acc.at[e], c_send.at[e], c_recv.at[e], partner)
        arrived(core_stats.at[e], cs_send.at[e], cs_recv.at[e], partner)
        for d in order:
            yy = (y + d) % Y
            merged = merge([own_acc[e, yy], core_acc[e, yy]], [own_stats[e, yy], core_stats[e, yy]], diagonal)
            if d == 0:
                put(y_in.at[0, e], y_in_stats.at[0, e], *merged)
            else:
                put(y_out.at[d, e], y_out_stats.at[d, e], *merged)
                there = at_seq(yy, z, c)
                copies.append(send(y_out.at[d, e], y_in.at[d, e], y_send.at[d, e], y_recv.at[d, e], there))
                copies.append(send(y_out_stats.at[d, e], y_in_stats.at[d, e], ys_send.at[d, e], ys_recv.at[d, e], there))
    for e in order:
        for d in (1, 3, 2):
            there = at_seq((y - d + Y) % Y, z, c)
            arrived(y_in.at[d, e], y_send.at[d, e], y_recv.at[d, e], there)
            arrived(y_in_stats.at[d, e], ys_send.at[d, e], ys_recv.at[d, e], there)
        merged = merge([y_in[d, e] for d in range(Y)], [y_in_stats[d, e] for d in range(Y)], diagonal)
        if e == 0:
            put(z_in.at[0], z_in_stats.at[0], *merged)
        else:
            put(z_out.at[e], z_out_stats.at[e], *merged)
            there = at_seq(y, (z + e) % Z, c)
            copies.append(send(z_out.at[e], z_in.at[e], z_send.at[e], z_recv.at[e], there))
            copies.append(send(z_out_stats.at[e], z_in_stats.at[e], zs_send.at[e], zs_recv.at[e], there))
    for e in (2, 1, 3):
        there = at_seq(y, (z - e + Z) % Z, c)
        arrived(z_in.at[e], z_send.at[e], z_recv.at[e], there)
        arrived(z_in_stats.at[e], zs_send.at[e], zs_recv.at[e], there)
    o, m, total = merge([z_in[e] for e in range(Z)], [z_in_stats[e] for e in range(Z)], diagonal)
    turned[...] = o / jnp.broadcast_to(total, (TILE, TILE)).T
    for i in range(HEADS):
        att[y, z, c, :, i * HD : (i + 1) * HD] = turned[pl.ds(i, ROWS, stride=HEADS), :].astype(BF16)
    gather = Gather(att, *sems)
    gather.start()
    for copy in copies:
        copy.wait_send()
    load_w.wait()
    near = 3 - 2 * (z % 2)
    far = Z - near
    for dy in (1, 3):
        gather.from_y(dy, 0)
    gather.from_z(near)
    gather.from_z(far)
    gather.from_y(2, 0)

    def exchange(to, pair):
        return pltpu.make_async_remote_copy(
            src_ref=part.at[to, pair], dst_ref=parts_in.at[h, pair], send_sem=h_send.at[to, pair], recv_sem=h_recv.at[h, pair],
            device_id={"head": to}, device_id_type=pl.DeviceIdType.MESH,
        )

    def project(dz):
        zz = (z - dz + Z) % Z
        pair = zz % 2
        rows = jnp.concatenate([att[yy, zz, j] for yy in range(Y) for j in range(C)], axis=0)
        share = dot(rows, w[...]).astype(BF16)
        for yy in range(Y):
            to = yy * 2 + zz // 2
            its = share[yy * C * ROWS : (yy + 1) * C * ROWS]

            @pl.when(to == h)
            def _():
                parts_in[h, pair] = its

            @pl.when(to != h)
            def _():
                part[to, pair] = its
                exchange(to, pair).start()

    for dy in range(Y):
        gather.from_core(dy, 0)
    project(0)
    gather.from_z(2)
    for dz in (near, far):
        for dy in (1, 3, 2):
            gather.from_y(dy, dz)
    for dz in (near, far):
        for dy in range(Y):
            gather.from_core(dy, dz)
        project(dz)
    for dy in (1, 3, 2):
        gather.from_y(dy, 2)
    for dy in range(Y):
        gather.from_core(dy, 2)
    project(2)
    gather.finish()
    for s in range(GROUPS):

        @pl.when(s != h)
        def _():
            for pair in range(2):
                arrived(parts_in.at[s, pair], h_send.at[s, pair], h_recv.at[s, pair], {"head": s})

    total = sum(parts_in[s].astype(F32) for s in range(GROUPS))
    out_ref[...] = total.reshape(out_ref.shape).astype(BF16)
    for s in range(GROUPS):

        @pl.when(s != h)
        def _():
            for pair in range(2):
                exchange(s, pair).wait_send()


def finish(pick, found, w):
    vmem = pl.BlockSpec(memory_space=VMEM)
    width = w.shape[1]
    rows = BATCH // GROUPS
    dma = pltpu.SemaphoreType.DMA
    return pl.pallas_call(
        finish_kernel,
        out_shape=jax.ShapeDtypeStruct((rows, width), BF16),
        in_specs=[pl.BlockSpec(memory_space=pltpu.SMEM), vmem, pl.BlockSpec(memory_space=pltpu.HBM)],
        out_specs=vmem,
        scratch_shapes=[
            VMEM((Z, Y, TILE, HD), BF16), VMEM((Z, Y, 2, HD), F32),
            VMEM((Z, Y, TILE, HD), BF16), VMEM((Z, Y, 2, HD), F32),
            VMEM((Z, Y, TILE, HD), BF16), VMEM((Z, Y, 2, HD), F32),
            VMEM((Y, Z, TILE, HD), BF16), VMEM((Y, Z, 2, HD), F32),
            VMEM((Y, Z, TILE, HD), BF16), VMEM((Y, Z, 2, HD), F32),
            VMEM((Z, TILE, HD), BF16), VMEM((Z, 2, HD), F32),
            VMEM((Z, TILE, HD), BF16), VMEM((Z, 2, HD), F32),
            VMEM((TILE, HD), F32),
            VMEM((Y, Z, C, ROWS, HEADS * HD), BF16),
            VMEM((HEADS * HD, width), BF16),
            VMEM((GROUPS, 2, rows // 2, width), BF16), VMEM((GROUPS, 2, rows // 2, width), BF16),
            dma,
            *[dma((Z,)) for _ in range(4)],
            *[dma((Y, Z)) for _ in range(4)],
            *[dma((Z,)) for _ in range(4)],
            dma((GROUPS, 2)), dma((GROUPS, 2)),
            *GATHER_SEMS,
        ],
        compiler_params=pltpu.CompilerParams(collective_id=1, has_side_effects=True, vmem_limit_bytes=12 << 20),
        name="finish",
    )(pick, found, w)


def shards(queries, cache, page_table, page_count, out_weight):
    cache = cache.reshape(2, PAGES, PAGE, HD)
    stay = functools.partial(pltpu.with_memory_space_constraint, memory_space=pltpu.HBM)
    q, pick, who, kt, v = prepare(stay(queries.reshape(TILE, HD)), stay(page_table.T), stay(page_count.reshape(1, BATCH)), stay(cache))
    found = attend(pick, who, q.reshape(BLOCKS, TILE, HD), kt, v)
    return finish(pick, found, stay(out_weight))


def solution(mesh):
    return jax.shard_map(
        shards,
        mesh=mesh,
        in_specs=(
            P("seq", "head", None),
            P(None, "seq", "head", None, None),
            P(),
            P(),
            P("head", "seq"),
        ),
        out_specs=P("head", "seq"),
        check_vma=False,
    )
```

```python
import functools
import math

import jax
import jax.numpy as jnp
from jax import lax
from jax.experimental import pallas as pl
from jax.experimental.pallas import tpu as pltpu
from jax.sharding import PartitionSpec as P

Y, Z, C = 4, 4, 2
BLOCKS = Y * Z * C
ROWS = 16
HEADS = 8
HD = 128
PAGE = 128
PAGES = 64
SLOTS = 64
BATCH = BLOCKS * ROWS
TILE = ROWS * HEADS
GROUPS = 8
CAP = 4
CHUNK = 8
UNROLL = 8
NONE = 2560
STEPS = NONE // CHUNK // UNROLL
LOWEST = -1000.0
LOG2E_SCALE = math.log2(math.e) / math.sqrt(HD)
F32, BF16 = jnp.float32, jnp.bfloat16
VMEM = pltpu.VMEM


def position():
    me = lax.axis_index("seq")
    return me // (Z * C), (me // C) % Z, me % C


def at_seq(y, z, c):
    return {"seq": (y * Z + z) * C + c}


def send(src, dst, send_sem, recv_sem, device):
    copy = pltpu.make_async_remote_copy(
        src_ref=src, dst_ref=dst, send_sem=send_sem, recv_sem=recv_sem,
        device_id=device, device_id_type=pl.DeviceIdType.MESH,
    )
    copy.start()
    return copy


def arrived(dst, send_sem, recv_sem, device):
    pltpu.make_async_remote_copy(
        src_ref=dst, dst_ref=dst, send_sem=send_sem, recv_sem=recv_sem,
        device_id=device, device_id_type=pl.DeviceIdType.MESH,
    ).wait_recv()


def seq_peers(y, z, c):
    peers = [at_seq(y, (z + d) % Z, c) for d in (2, 1, 3)]
    peers += [at_seq(y, z, 1 - c)]
    peers += [at_seq((y + d) % Y, z, c) for d in range(1, Y)]
    return peers


def greet(peers, meanwhile=None):
    barrier = pltpu.get_barrier_semaphore()
    for peer in peers:
        pl.semaphore_signal(barrier, inc=1, device_id=peer, device_id_type=pl.DeviceIdType.MESH)
    if meanwhile is not None:
        meanwhile()
    pl.semaphore_wait(barrier, len(peers))


class Gather:
    def __init__(self, buf, zs, zr, ys, yr, ds, dr):
        self.buf, self.sems = buf, (zs, zr, ys, yr, ds, dr)
        self.y, self.z, self.c = position()
        self.copies = []

    def block(self, dy, dz, other=False):
        y, z = (self.y - dy + Y) % Y, (self.z - dz + Z) % Z
        c = 1 - self.c if other else self.c
        return self.buf.at[y, z, c]

    def send(self, block, send_sem, recv_sem, y, z, c):
        self.copies.append(send(block, block, send_sem, recv_sem, at_seq((y + Y) % Y, (z + Z) % Z, c)))

    def to_core(self, dy, dz):
        ds, dr = self.sems[4:]
        self.send(self.block(dy, dz), ds.at[dy, dz], dr.at[dy, dz], self.y, self.z, 1 - self.c)

    def along_y(self, dz):
        ys, yr = self.sems[2:4]
        for dy in (2, 1, 3):
            self.send(self.block(0, dz), ys.at[dy, dz], yr.at[dy, dz], self.y + dy, self.z, self.c)

    def start(self):
        zs, zr = self.sems[:2]
        for dz in (2, 1, 3):
            self.send(self.block(0, 0), zs.at[dz], zr.at[dz], self.y, self.z + dz, self.c)
        self.along_y(0)
        self.to_core(0, 0)

    def from_z(self, dz):
        zs, zr = self.sems[:2]
        arrived(self.block(0, dz), zs.at[dz], zr.at[dz], at_seq(self.y, (self.z - dz + Z) % Z, self.c))
        self.along_y(dz)
        self.to_core(0, dz)

    def from_y(self, dy, dz):
        ys, yr = self.sems[2:4]
        arrived(self.block(dy, dz), ys.at[dy, dz], yr.at[dy, dz], at_seq((self.y - dy + Y) % Y, self.z, self.c))
        self.to_core(dy, dz)

    def from_core(self, dy, dz):
        ds, dr = self.sems[4:]
        arrived(self.block(dy, dz, other=True), ds.at[dy, dz], dr.at[dy, dz], at_seq(self.y, self.z, 1 - self.c))

    def finish(self):
        for copy in self.copies:
            copy.wait_send()


GATHER_SEMS = [
    pltpu.SemaphoreType.DMA((Z,)), pltpu.SemaphoreType.DMA((Z,)),
    pltpu.SemaphoreType.DMA((Y, Z)), pltpu.SemaphoreType.DMA((Y, Z)),
    pltpu.SemaphoreType.DMA((Y, Z)), pltpu.SemaphoreType.DMA((Y, Z)),
]


def dot(a, b, dims=((1,), (0,))):
    return lax.dot_general(a, b, (dims, ((), ())), preferred_element_type=F32)


def square(n, f):
    return f(lax.broadcasted_iota(jnp.int32, (n, n), 0), lax.broadcasted_iota(jnp.int32, (n, n), 1)).astype(F32).astype(BF16)


def selection(table, counts):
    own = lax.axis_index("seq")
    page = (table % PAGES).astype(F32)
    slot = lax.broadcasted_iota(jnp.int32, (SLOTS, BATCH), 0)
    present = (slot < counts) & (table // PAGES == own)
    rank = dot(square(SLOTS, jnp.greater_equal), present.astype(F32).astype(BF16))
    picks = [jnp.sum(jnp.where(present & (rank == k + 1.0), page + 1.0, 0.0), axis=0, keepdims=True) for k in range(CAP)]
    number = lax.broadcasted_iota(jnp.int32, (PAGES, BATCH), 0).astype(F32)
    takes = [number + 1.0 == pick for pick in picks]
    taken = sum(take.astype(F32) for take in takes)
    before = dot(taken.astype(BF16), square(BATCH, jnp.less_equal))
    chunks = jnp.floor((jnp.sum(taken, axis=1, keepdims=True) + (CHUNK - 1.0)) * (1.0 / CHUNK))
    first = dot(square(PAGES, jnp.greater), jnp.broadcast_to(chunks, (PAGES, 128)).astype(BF16))[:, 0:1]
    place = first * CHUNK + before - 1.0
    places = [
        jnp.where(pick > 0.0, jnp.sum(jnp.where(take, place, 0.0), axis=0, keepdims=True), float(NONE))
        for pick, take in zip(picks, takes)
    ]
    total = jnp.sum(chunks, axis=0, keepdims=True)
    group = lax.broadcasted_iota(jnp.int32, (BLOCKS, BATCH), 0)
    mine = group == lax.broadcasted_iota(jnp.int32, (BLOCKS, BATCH), 1) // ROWS
    column = lax.broadcasted_iota(jnp.int32, (BATCH, 128), 1)
    within = lax.broadcasted_iota(jnp.int32, (BATCH, 128), 0) % ROWS
    high = jnp.zeros((BLOCKS, 128), F32)
    low = jnp.zeros((BLOCKS, 128), F32)
    for k, p in enumerate(places):
        put = (column == k * ROWS + within).astype(F32).astype(BF16)
        upper = jnp.floor(p * (1.0 / 16.0))
        high += dot(jnp.where(mine, upper, 0.0).astype(BF16), put)
        low += dot(jnp.where(mine, p - upper * 16.0, 0.0).astype(BF16), put)
    lane = lax.broadcasted_iota(jnp.int32, (BLOCKS, 128), 1)
    pick = jnp.where(lane == CAP * ROWS, total, high * 16.0 + low)
    chunk = lax.broadcasted_iota(jnp.int32, (PAGES, BATCH), 1).astype(F32)
    page_of = jnp.sum(jnp.where((first <= chunk) & (chunk < first + chunks), number, 0.0), axis=0, keepdims=True)
    step = lax.broadcasted_iota(jnp.int32, (STEPS, BATCH), 0)
    its = step == lax.broadcasted_iota(jnp.int32, (STEPS, BATCH), 1) // UNROLL
    put = (column == 64 + lax.broadcasted_iota(jnp.int32, (BATCH, 128), 0) % UNROLL).astype(F32).astype(BF16)
    pages = dot(jnp.where(its, page_of, 0.0).astype(BF16), put)
    return places, pick.astype(jnp.int32), pages.astype(jnp.int32)


def owners(places, start):
    at = lax.broadcasted_iota(jnp.int32, (256, BATCH), 0).astype(F32) + start.astype(F32)
    hit = (at == places[0:1]) | (at == places[1:2]) | (at == places[2:3]) | (at == places[3:4])
    who = lax.broadcasted_iota(jnp.int32, (8, BATCH), 1)
    digit = jnp.where(lax.broadcasted_iota(jnp.int32, (8, BATCH), 0) == 0, who // 16, who % 16)
    digits = dot(digit.astype(F32).astype(BF16), jnp.where(hit, 1.0, 0.0).astype(BF16), ((1,), (1,)))
    return (digits[0:1] * 16.0 + digits[1:2]).astype(jnp.int32)


def prepare_kernel(
    q_ref, table_ref, counts_ref, cache_ref, all_ref, pick_ref, who_ref, kt_ref, v_ref,
    table, counts, keys, places, pages, in_sems, key_sems, *sems,
):
    y, z, c = position()
    half = PAGES // 2
    small = [
        pltpu.make_async_copy(q_ref, all_ref.at[y, z, c], in_sems.at[0]),
        pltpu.make_async_copy(table_ref, table, in_sems.at[1]),
        pltpu.make_async_copy(counts_ref, counts, in_sems.at[2]),
    ]
    loads = [
        pltpu.make_async_copy(cache_ref.at[0, pl.ds(i * half, half)], keys.at[pl.ds(i * half, half)], key_sems.at[i])
        for i in range(2)
    ]
    load_v = pltpu.make_async_copy(cache_ref.at[1], v_ref, in_sems.at[3])
    for load in small + loads:
        load.start()
    greet(seq_peers(y, z, c))
    small[0].wait()
    gather = Gather(all_ref, *sems)
    gather.start()
    load_v.start()
    small[1].wait()
    small[2].wait()
    rows, pick_ref[...], pages[...] = selection(table[...], counts[...])
    for k in range(CAP):
        places[k : k + 1] = rows[k]

    def turn(i, carry):
        for j in range(4):
            kt_ref[i * 4 + j] = keys[i * 4 + j].T
        return carry

    def name(i, carry):
        lane = lax.broadcasted_iota(jnp.int32, (1, 128), 1)
        who = owners(places, i * 256)
        for j in range(2):
            half_row = who[:, j * 128 : (j + 1) * 128]
            rolled = pltpu.roll(jnp.broadcast_to(half_row, (8, 128)), 64, 1)[0:1]
            row = 4 * i + 2 * j
            who_ref[pl.ds(row, 1)] = jnp.where(lane < 64, half_row, pages[pl.ds(row, 1)])
            who_ref[pl.ds(row + 1, 1)] = jnp.where(lane < 64, rolled, pages[pl.ds(row + 1, 1)])
        return carry

    loads[0].wait()
    lax.fori_loop(0, 8, turn, 0)
    for dz in (1, 3, 2):
        gather.from_z(dz)
    loads[1].wait()
    lax.fori_loop(8, 16, turn, 0)
    lax.fori_loop(0, NONE // 256, name, 0)
    for dz in (0, 1, 3, 2):
        for dy in (1, 3, 2):
            gather.from_y(dy, dz)
    for dz in (0, 1, 3, 2):
        for dy in range(Y):
            gather.from_core(dy, dz)
    gather.finish()
    load_v.wait()


def prepare(q, table, counts, cache):
    vmem = pl.BlockSpec(memory_space=VMEM)
    hbm = pl.BlockSpec(memory_space=pltpu.HBM)
    return pl.pallas_call(
        prepare_kernel,
        out_shape=(
            jax.ShapeDtypeStruct((Y, Z, C, TILE, HD), BF16),
            jax.ShapeDtypeStruct((BLOCKS, 128), jnp.int32),
            jax.ShapeDtypeStruct((STEPS, 128), jnp.int32),
            jax.ShapeDtypeStruct((PAGES, HD, PAGE), BF16),
            jax.ShapeDtypeStruct((PAGES, PAGE, HD), BF16),
        ),
        in_specs=[hbm, hbm, hbm, hbm],
        out_specs=(vmem,) * 5,
        scratch_shapes=[
            VMEM((SLOTS, BATCH), jnp.int32),
            VMEM((1, BATCH), jnp.int32),
            VMEM((PAGES, PAGE, HD), BF16),
            VMEM((8, BATCH), F32),
            VMEM((STEPS, 128), jnp.int32),
            pltpu.SemaphoreType.DMA((4,)),
            pltpu.SemaphoreType.DMA((2,)),
            *GATHER_SEMS,
        ],
        compiler_params=pltpu.CompilerParams(collective_id=0, has_side_effects=True, vmem_limit_bytes=12 << 20),
        name="prepare",
    )(q, table, counts, cache)


def attend_kernel(pick_in, who_in, q_in, kt, v, found, q, scores, pick, who, sems):
    tables = [pltpu.make_async_copy(pick_in, pick, sems.at[0]), pltpu.make_async_copy(who_in, who, sems.at[1])]
    for table in tables:
        table.start()

    def widen(i, carry):
        for j in range(4):
            q[pl.ds((i * 4 + j) * ROWS, ROWS)] = q_in[i * 4 + j].astype(F32).reshape(ROWS, HEADS, HD)
        return carry

    lax.fori_loop(0, BLOCKS // 4, widen, 0)
    found[pl.ds(NONE, 8), 0] = jnp.zeros((8, HEADS, HD), F32)
    found[pl.ds(NONE, 8), 1] = jnp.full((8, HEADS, HD), -1e30, F32)
    ones = jnp.ones((PAGE, HD), BF16)
    for table in tables:
        table.wait()

    def scores_of(g):
        for u in range(UNROLL):
            left = jnp.concatenate([q[who[g, u * CHUNK + j]] for j in range(CHUNK)], axis=0).astype(BF16)
            scores[u] = dot(left, kt[who[g, 64 + u]])

    def weigh(g):
        for u in range(UNROLL):
            at = pl.ds((g * UNROLL + u) * CHUNK, CHUNK)
            s = scores[u] * LOG2E_SCALE
            m = jnp.max(s, axis=1, keepdims=True)
            w = jnp.exp2(s - m).astype(BF16)
            o = dot(w, jnp.concatenate([v[who[g, 64 + u]], ones], axis=1))
            total = o[:, HD:]
            found[at, 0] = (o[:, :HD] / total).reshape(CHUNK, HEADS, HD)
            found[at, 1] = (m + jnp.log2(total)).reshape(CHUNK, HEADS, HD)

    scores_of(0)
    steps = (pick[0, CAP * ROWS] + UNROLL - 1) // UNROLL

    def step(g, carry):
        weigh(g)
        scores_of(jnp.minimum(g + 1, STEPS - 1))
        return carry

    lax.fori_loop(0, steps, step, 0)


def attend(pick, who, q, kt, v):
    vmem = pl.BlockSpec(memory_space=VMEM)
    return pl.pallas_call(
        attend_kernel,
        out_shape=VMEM((NONE + 8, 2, HEADS, HD), F32),
        in_specs=[vmem] * 5,
        out_specs=vmem,
        scratch_shapes=[
            VMEM((BATCH, HEADS, HD), F32),
            VMEM((UNROLL, CHUNK * HEADS, PAGE), F32),
            pltpu.SMEM((BLOCKS, 128), jnp.int32),
            pltpu.SMEM((STEPS, 128), jnp.int32),
            pltpu.SemaphoreType.DMA((2,)),
        ],
        compiler_params=pltpu.CompilerParams(vmem_limit_bytes=8 << 20),
        name="attend",
    )(pick, who, q, kt, v)


def settle(pick, found, g, values, stats):
    sublane = lax.broadcasted_iota(jnp.int32, (HEADS, HD), 0)
    lane = lax.broadcasted_iota(jnp.int32, (HEADS, HD), 1)
    tops = jnp.zeros((HEADS, HD), F32)
    totals = jnp.zeros((HEADS, HD), F32)
    outs = []
    for s in range(ROWS):
        at = [pick[g, k * ROWS + s] for k in range(CAP)]
        highest = [found[p, 1] for p in at]
        m = jnp.maximum(jnp.floor(functools.reduce(jnp.maximum, highest) * 0.5 + 0.5) * 2.0, LOWEST)
        factors = [jnp.exp2(t - m) for t in highest]
        outs.append(sum(f * found[p, 0] for f, p in zip(factors, at)))
        here = lane - sublane == s * HEADS
        tops = jnp.where(here, m, tops)
        totals = jnp.where(here, sum(factors), totals)
    stats[0:1] = jnp.sum(tops, axis=0, keepdims=True)
    stats[1:2] = jnp.sum(totals, axis=0, keepdims=True)
    values[...] = jnp.concatenate(outs, axis=0).astype(BF16)


def merge(parts, stats, diagonal):
    m = functools.reduce(jnp.maximum, [s[0:1] for s in stats])
    factors = [jnp.exp2(s[0:1] - m) for s in stats]
    total = sum(s[1:2] * f for s, f in zip(stats, factors))
    left = jnp.concatenate([jnp.where(diagonal, jnp.broadcast_to(f, (TILE, TILE)), 0.0).astype(BF16) for f in factors], axis=1)
    return dot(left, jnp.concatenate(parts, axis=0)), m, total


def finish_kernel(
    pick, found, w_ref, out_ref,
    own_acc, own_stats, their_acc, their_stats,
    core_acc, core_stats, y_out, y_out_stats, y_in, y_in_stats, z_out, z_out_stats, z_in, z_in_stats,
    turned, att, w, part, parts_in, w_sem,
    c_send, c_recv, cs_send, cs_recv, y_send, y_recv, ys_send, ys_recv, z_send, z_recv, zs_send, zs_recv, h_send, h_recv, *sems,
):
    y, z, c = position()
    h = lax.axis_index("head")
    other = 1 - c
    load_w = pltpu.make_async_copy(w_ref, w, w_sem)
    load_w.start()
    partner = at_seq(y, z, other)
    order = (2, 1, 3, 0)

    def settle_all(e, core, values, stats):
        def one(yy, carry):
            settle(pick, found, (yy * Z + (z + e) % Z) * C + core, values.at[e, yy], stats.at[e, yy])
            return carry

        lax.fori_loop(0, Y, one, 0)

    def early():
        for e in order:
            settle_all(e, other, their_acc, their_stats)
        settle_all(order[0], c, own_acc, own_stats)

    greet(seq_peers(y, z, c) + [{"head": (h + d) % GROUPS} for d in range(1, GROUPS)], early)
    copies = []
    for e in order:
        copies.append(send(their_acc.at[e], core_acc.at[e], c_send.at[e], c_recv.at[e], partner))
        copies.append(send(their_stats.at[e], core_stats.at[e], cs_send.at[e], cs_recv.at[e], partner))
    diagonal = lax.broadcasted_iota(jnp.int32, (TILE, TILE), 0) == lax.broadcasted_iota(jnp.int32, (TILE, TILE), 1)

    def put(values, rows, o, m, total):
        values[...] = o.astype(BF16)
        rows[0:1] = m
        rows[1:2] = total

    for e in order:
        if e != order[0]:
            settle_all(e, c, own_acc, own_stats)
        arrived(core_acc.at[e], c_send.at[e], c_recv.at[e], partner)
        arrived(core_stats.at[e], cs_send.at[e], cs_recv.at[e], partner)
        for d in order:
            yy = (y + d) % Y
            merged = merge([own_acc[e, yy], core_acc[e, yy]], [own_stats[e, yy], core_stats[e, yy]], diagonal)
            if d == 0:
                put(y_in.at[0, e], y_in_stats.at[0, e], *merged)
            else:
                put(y_out.at[d, e], y_out_stats.at[d, e], *merged)
                there = at_seq(yy, z, c)
                copies.append(send(y_out.at[d, e], y_in.at[d, e], y_send.at[d, e], y_recv.at[d, e], there))
                copies.append(send(y_out_stats.at[d, e], y_in_stats.at[d, e], ys_send.at[d, e], ys_recv.at[d, e], there))
    for e in order:
        for d in (1, 3, 2):
            there = at_seq((y - d + Y) % Y, z, c)
            arrived(y_in.at[d, e], y_send.at[d, e], y_recv.at[d, e], there)
            arrived(y_in_stats.at[d, e], ys_send.at[d, e], ys_recv.at[d, e], there)
        merged = merge([y_in[d, e] for d in range(Y)], [y_in_stats[d, e] for d in range(Y)], diagonal)
        if e == 0:
            put(z_in.at[0], z_in_stats.at[0], *merged)
        else:
            put(z_out.at[e], z_out_stats.at[e], *merged)
            there = at_seq(y, (z + e) % Z, c)
            copies.append(send(z_out.at[e], z_in.at[e], z_send.at[e], z_recv.at[e], there))
            copies.append(send(z_out_stats.at[e], z_in_stats.at[e], zs_send.at[e], zs_recv.at[e], there))
    for e in (2, 1, 3):
        there = at_seq(y, (z - e + Z) % Z, c)
        arrived(z_in.at[e], z_send.at[e], z_recv.at[e], there)
        arrived(z_in_stats.at[e], zs_send.at[e], zs_recv.at[e], there)
    o, m, total = merge([z_in[e] for e in range(Z)], [z_in_stats[e] for e in range(Z)], diagonal)
    turned[...] = o / jnp.broadcast_to(total, (TILE, TILE)).T
    for i in range(HEADS):
        att[y, z, c, :, i * HD : (i + 1) * HD] = turned[pl.ds(i, ROWS, stride=HEADS), :].astype(BF16)
    gather = Gather(att, *sems)
    gather.start()
    for copy in copies:
        copy.wait_send()
    load_w.wait()
    near = 3 - 2 * (z % 2)
    far = Z - near
    for dy in (1, 3):
        gather.from_y(dy, 0)
    gather.from_z(near)
    gather.from_z(far)
    gather.from_y(2, 0)

    def exchange(to, pair):
        return pltpu.make_async_remote_copy(
            src_ref=part.at[to, pair], dst_ref=parts_in.at[h, pair], send_sem=h_send.at[to, pair], recv_sem=h_recv.at[h, pair],
            device_id={"head": to}, device_id_type=pl.DeviceIdType.MESH,
        )

    def project(dz):
        zz = (z - dz + Z) % Z
        pair = zz % 2
        rows = jnp.concatenate([att[yy, zz, j] for yy in range(Y) for j in range(C)], axis=0)
        share = dot(rows, w[...]).astype(BF16)
        for yy in range(Y):
            to = yy * 2 + zz // 2
            its = share[yy * C * ROWS : (yy + 1) * C * ROWS]

            @pl.when(to == h)
            def _():
                parts_in[h, pair] = its

            @pl.when(to != h)
            def _():
                part[to, pair] = its
                exchange(to, pair).start()

    for dy in range(Y):
        gather.from_core(dy, 0)
    project(0)
    gather.from_z(2)
    for dz in (near, far):
        for dy in (1, 3, 2):
            gather.from_y(dy, dz)
    for dz in (near, far):
        for dy in range(Y):
            gather.from_core(dy, dz)
        project(dz)
    for dy in (1, 3, 2):
        gather.from_y(dy, 2)
    for dy in range(Y):
        gather.from_core(dy, 2)
    project(2)
    gather.finish()
    for s in range(GROUPS):

        @pl.when(s != h)
        def _():
            for pair in range(2):
                arrived(parts_in.at[s, pair], h_send.at[s, pair], h_recv.at[s, pair], {"head": s})

    total = sum(parts_in[s].astype(F32) for s in range(GROUPS))
    out_ref[...] = total.reshape(out_ref.shape).astype(BF16)
    for s in range(GROUPS):

        @pl.when(s != h)
        def _():
            for pair in range(2):
                exchange(s, pair).wait_send()


def finish(pick, found, w):
    vmem = pl.BlockSpec(memory_space=VMEM)
    width = w.shape[1]
    rows = BATCH // GROUPS
    dma = pltpu.SemaphoreType.DMA
    return pl.pallas_call(
        finish_kernel,
        out_shape=jax.ShapeDtypeStruct((rows, width), BF16),
        in_specs=[pl.BlockSpec(memory_space=pltpu.SMEM), vmem, pl.BlockSpec(memory_space=pltpu.HBM)],
        out_specs=vmem,
        scratch_shapes=[
            VMEM((Z, Y, TILE, HD), BF16), VMEM((Z, Y, 2, HD), F32),
            VMEM((Z, Y, TILE, HD), BF16), VMEM((Z, Y, 2, HD), F32),
            VMEM((Z, Y, TILE, HD), BF16), VMEM((Z, Y, 2, HD), F32),
            VMEM((Y, Z, TILE, HD), BF16), VMEM((Y, Z, 2, HD), F32),
            VMEM((Y, Z, TILE, HD), BF16), VMEM((Y, Z, 2, HD), F32),
            VMEM((Z, TILE, HD), BF16), VMEM((Z, 2, HD), F32),
            VMEM((Z, TILE, HD), BF16), VMEM((Z, 2, HD), F32),
            VMEM((TILE, HD), F32),
            VMEM((Y, Z, C, ROWS, HEADS * HD), BF16),
            VMEM((HEADS * HD, width), BF16),
            VMEM((GROUPS, 2, rows // 2, width), BF16), VMEM((GROUPS, 2, rows // 2, width), BF16),
            dma,
            *[dma((Z,)) for _ in range(4)],
            *[dma((Y, Z)) for _ in range(4)],
            *[dma((Z,)) for _ in range(4)],
            dma((GROUPS, 2)), dma((GROUPS, 2)),
            *GATHER_SEMS,
        ],
        compiler_params=pltpu.CompilerParams(collective_id=1, has_side_effects=True, vmem_limit_bytes=12 << 20),
        name="finish",
    )(pick, found, w)


def shards(queries, cache, page_table, page_count, out_weight):
    cache = cache.reshape(2, PAGES, PAGE, HD)
    stay = functools.partial(pltpu.with_memory_space_constraint, memory_space=pltpu.HBM)
    q, pick, who, kt, v = prepare(stay(queries.reshape(TILE, HD)), stay(page_table.T), stay(page_count.reshape(1, BATCH)), stay(cache))
    found = attend(pick, who, q.reshape(BLOCKS, TILE, HD), kt, v)
    return finish(pick, found, stay(out_weight))


def solution(mesh):
    return jax.shard_map(
        shards,
        mesh=mesh,
        in_specs=(
            P("seq", "head", None),
            P(None, "seq", "head", None, None),
            P(),
            P(),
            P("head", "seq"),
        ),
        out_specs=P("head", "seq"),
        check_vma=False,
    )
```

```python
import functools
import math

import jax
import jax.numpy as jnp
from jax import lax
from jax.experimental import pallas as pl
from jax.experimental.pallas import tpu as pltpu
from jax.sharding import PartitionSpec as P

Y, Z, C = 4, 4, 2
BLOCKS = Y * Z * C
ROWS = 16
HEADS = 8
HD = 128
PAGE = 128
PAGES = 64
SLOTS = 64
BATCH = BLOCKS * ROWS
TILE = ROWS * HEADS
GROUPS = 8
CAP = 4
CHUNK = 8
UNROLL = 8
NONE = 2560
STEPS = NONE // CHUNK // UNROLL
LOWEST = -1000.0
LOG2E_SCALE = math.log2(math.e) / math.sqrt(HD)
F32, BF16 = jnp.float32, jnp.bfloat16
VMEM = pltpu.VMEM


def position():
    me = lax.axis_index("seq")
    return me // (Z * C), (me // C) % Z, me % C


def at_seq(y, z, c):
    return {"seq": (y * Z + z) * C + c}


def send(src, dst, send_sem, recv_sem, device):
    copy = pltpu.make_async_remote_copy(
        src_ref=src, dst_ref=dst, send_sem=send_sem, recv_sem=recv_sem,
        device_id=device, device_id_type=pl.DeviceIdType.MESH,
    )
    copy.start()
    return copy


def arrived(dst, send_sem, recv_sem, device):
    pltpu.make_async_remote_copy(
        src_ref=dst, dst_ref=dst, send_sem=send_sem, recv_sem=recv_sem,
        device_id=device, device_id_type=pl.DeviceIdType.MESH,
    ).wait_recv()


def seq_peers(y, z, c):
    peers = [at_seq(y, (z + d) % Z, c) for d in (2, 1, 3)]
    peers += [at_seq(y, z, 1 - c)]
    peers += [at_seq((y + d) % Y, z, c) for d in range(1, Y)]
    return peers


def greet(peers, meanwhile=None):
    barrier = pltpu.get_barrier_semaphore()
    for peer in peers:
        pl.semaphore_signal(barrier, inc=1, device_id=peer, device_id_type=pl.DeviceIdType.MESH)
    if meanwhile is not None:
        meanwhile()
    pl.semaphore_wait(barrier, len(peers))


class Gather:
    def __init__(self, buf, zs, zr, ys, yr, ds, dr):
        self.buf, self.sems = buf, (zs, zr, ys, yr, ds, dr)
        self.y, self.z, self.c = position()
        self.copies = []

    def block(self, dy, dz, other=False):
        y, z = (self.y - dy + Y) % Y, (self.z - dz + Z) % Z
        c = 1 - self.c if other else self.c
        return self.buf.at[y, z, c]

    def send(self, block, send_sem, recv_sem, y, z, c):
        self.copies.append(send(block, block, send_sem, recv_sem, at_seq((y + Y) % Y, (z + Z) % Z, c)))

    def to_core(self, dy, dz):
        ds, dr = self.sems[4:]
        self.send(self.block(dy, dz), ds.at[dy, dz], dr.at[dy, dz], self.y, self.z, 1 - self.c)

    def along_y(self, dz):
        ys, yr = self.sems[2:4]
        for dy in (2, 1, 3):
            self.send(self.block(0, dz), ys.at[dy, dz], yr.at[dy, dz], self.y + dy, self.z, self.c)

    def start(self):
        zs, zr = self.sems[:2]
        for dz in (2, 1, 3):
            self.send(self.block(0, 0), zs.at[dz], zr.at[dz], self.y, self.z + dz, self.c)
        self.along_y(0)
        self.to_core(0, 0)

    def from_z(self, dz):
        zs, zr = self.sems[:2]
        arrived(self.block(0, dz), zs.at[dz], zr.at[dz], at_seq(self.y, (self.z - dz + Z) % Z, self.c))
        self.along_y(dz)
        self.to_core(0, dz)

    def from_y(self, dy, dz):
        ys, yr = self.sems[2:4]
        arrived(self.block(dy, dz), ys.at[dy, dz], yr.at[dy, dz], at_seq((self.y - dy + Y) % Y, self.z, self.c))
        self.to_core(dy, dz)

    def from_core(self, dy, dz):
        ds, dr = self.sems[4:]
        arrived(self.block(dy, dz, other=True), ds.at[dy, dz], dr.at[dy, dz], at_seq(self.y, self.z, 1 - self.c))

    def finish(self):
        for copy in self.copies:
            copy.wait_send()


GATHER_SEMS = [
    pltpu.SemaphoreType.DMA((Z,)), pltpu.SemaphoreType.DMA((Z,)),
    pltpu.SemaphoreType.DMA((Y, Z)), pltpu.SemaphoreType.DMA((Y, Z)),
    pltpu.SemaphoreType.DMA((Y, Z)), pltpu.SemaphoreType.DMA((Y, Z)),
]


def dot(a, b, dims=((1,), (0,))):
    return lax.dot_general(a, b, (dims, ((), ())), preferred_element_type=F32)


def square(n, f):
    return f(lax.broadcasted_iota(jnp.int32, (n, n), 0), lax.broadcasted_iota(jnp.int32, (n, n), 1)).astype(F32).astype(BF16)


def selection(table, counts):
    own = lax.axis_index("seq")
    page = (table % PAGES).astype(F32)
    slot = lax.broadcasted_iota(jnp.int32, (SLOTS, BATCH), 0)
    present = (slot < counts) & (table // PAGES == own)
    rank = dot(square(SLOTS, jnp.greater_equal), present.astype(F32).astype(BF16))
    picks = [jnp.sum(jnp.where(present & (rank == k + 1.0), page + 1.0, 0.0), axis=0, keepdims=True) for k in range(CAP)]
    number = lax.broadcasted_iota(jnp.int32, (PAGES, BATCH), 0).astype(F32)
    takes = [number + 1.0 == pick for pick in picks]
    taken = sum(take.astype(F32) for take in takes)
    before = dot(taken.astype(BF16), square(BATCH, jnp.less_equal))
    chunks = jnp.floor((jnp.sum(taken, axis=1, keepdims=True) + (CHUNK - 1.0)) * (1.0 / CHUNK))
    first = dot(square(PAGES, jnp.greater), jnp.broadcast_to(chunks, (PAGES, 128)).astype(BF16))[:, 0:1]
    place = first * CHUNK + before - 1.0
    places = [
        jnp.where(pick > 0.0, jnp.sum(jnp.where(take, place, 0.0), axis=0, keepdims=True), float(NONE))
        for pick, take in zip(picks, takes)
    ]
    total = jnp.sum(chunks, axis=0, keepdims=True)
    group = lax.broadcasted_iota(jnp.int32, (BLOCKS, BATCH), 0)
    mine = group == lax.broadcasted_iota(jnp.int32, (BLOCKS, BATCH), 1) // ROWS
    column = lax.broadcasted_iota(jnp.int32, (BATCH, 128), 1)
    within = lax.broadcasted_iota(jnp.int32, (BATCH, 128), 0) % ROWS
    high = jnp.zeros((BLOCKS, 128), F32)
    low = jnp.zeros((BLOCKS, 128), F32)
    for k, p in enumerate(places):
        put = (column == k * ROWS + within).astype(F32).astype(BF16)
        upper = jnp.floor(p * (1.0 / 16.0))
        high += dot(jnp.where(mine, upper, 0.0).astype(BF16), put)
        low += dot(jnp.where(mine, p - upper * 16.0, 0.0).astype(BF16), put)
    lane = lax.broadcasted_iota(jnp.int32, (BLOCKS, 128), 1)
    pick = jnp.where(lane == CAP * ROWS, total, high * 16.0 + low)
    chunk = lax.broadcasted_iota(jnp.int32, (PAGES, BATCH), 1).astype(F32)
    page_of = jnp.sum(jnp.where((first <= chunk) & (chunk < first + chunks), number, 0.0), axis=0, keepdims=True)
    step = lax.broadcasted_iota(jnp.int32, (STEPS, BATCH), 0)
    its = step == lax.broadcasted_iota(jnp.int32, (STEPS, BATCH), 1) // UNROLL
    put = (column == 64 + lax.broadcasted_iota(jnp.int32, (BATCH, 128), 0) % UNROLL).astype(F32).astype(BF16)
    pages = dot(jnp.where(its, page_of, 0.0).astype(BF16), put)
    return places, pick.astype(jnp.int32), pages.astype(jnp.int32)


def owners(places, start):
    at = lax.broadcasted_iota(jnp.int32, (256, BATCH), 0).astype(F32) + start.astype(F32)
    hit = (at == places[0:1]) | (at == places[1:2]) | (at == places[2:3]) | (at == places[3:4])
    who = lax.broadcasted_iota(jnp.int32, (8, BATCH), 1)
    digit = jnp.where(lax.broadcasted_iota(jnp.int32, (8, BATCH), 0) == 0, who // 16, who % 16)
    digits = dot(digit.astype(F32).astype(BF16), jnp.where(hit, 1.0, 0.0).astype(BF16), ((1,), (1,)))
    return (digits[0:1] * 16.0 + digits[1:2]).astype(jnp.int32)


def prepare_kernel(
    q_ref, table_ref, counts_ref, cache_ref, all_ref, pick_ref, who_ref, kt_ref, v_ref,
    table, counts, keys, places, pages, in_sems, key_sems, *sems,
):
    y, z, c = position()
    half = PAGES // 2
    small = [
        pltpu.make_async_copy(q_ref, all_ref.at[y, z, c], in_sems.at[0]),
        pltpu.make_async_copy(table_ref, table, in_sems.at[1]),
        pltpu.make_async_copy(counts_ref, counts, in_sems.at[2]),
    ]
    loads = [
        pltpu.make_async_copy(cache_ref.at[0, pl.ds(i * half, half)], keys.at[pl.ds(i * half, half)], key_sems.at[i])
        for i in range(2)
    ]
    load_v = pltpu.make_async_copy(cache_ref.at[1], v_ref, in_sems.at[3])
    for load in small + loads:
        load.start()
    greet(seq_peers(y, z, c))
    small[0].wait()
    gather = Gather(all_ref, *sems)
    gather.start()
    load_v.start()
    small[1].wait()
    small[2].wait()
    rows, pick_ref[...], pages[...] = selection(table[...], counts[...])
    for k in range(CAP):
        places[k : k + 1] = rows[k]

    def turn(i, carry):
        for j in range(4):
            kt_ref[i * 4 + j] = keys[i * 4 + j].T
        return carry

    def name(i, carry):
        lane = lax.broadcasted_iota(jnp.int32, (1, 128), 1)
        who = owners(places, i * 256)
        for j in range(2):
            half_row = who[:, j * 128 : (j + 1) * 128]
            rolled = pltpu.roll(jnp.broadcast_to(half_row, (8, 128)), 64, 1)[0:1]
            row = 4 * i + 2 * j
            who_ref[pl.ds(row, 1)] = jnp.where(lane < 64, half_row, pages[pl.ds(row, 1)])
            who_ref[pl.ds(row + 1, 1)] = jnp.where(lane < 64, rolled, pages[pl.ds(row + 1, 1)])
        return carry

    loads[0].wait()
    lax.fori_loop(0, 8, turn, 0)
    for dz in (1, 3, 2):
        gather.from_z(dz)
    loads[1].wait()
    lax.fori_loop(8, 16, turn, 0)
    lax.fori_loop(0, NONE // 256, name, 0)
    for dz in (0, 1, 3, 2):
        for dy in (1, 3, 2):
            gather.from_y(dy, dz)
    gather.finish()
    for dz in (0, 1, 3, 2):
        for dy in range(Y):
            gather.from_core(dy, dz)
    load_v.wait()


def prepare(q, table, counts, cache):
    vmem = pl.BlockSpec(memory_space=VMEM)
    hbm = pl.BlockSpec(memory_space=pltpu.HBM)
    return pl.pallas_call(
        prepare_kernel,
        out_shape=(
            jax.ShapeDtypeStruct((Y, Z, C, TILE, HD), BF16),
            jax.ShapeDtypeStruct((BLOCKS, 128), jnp.int32),
            jax.ShapeDtypeStruct((STEPS, 128), jnp.int32),
            jax.ShapeDtypeStruct((PAGES, HD, PAGE), BF16),
            jax.ShapeDtypeStruct((PAGES, PAGE, HD), BF16),
        ),
        in_specs=[hbm, hbm, hbm, hbm],
        out_specs=(vmem,) * 5,
        scratch_shapes=[
            VMEM((SLOTS, BATCH), jnp.int32),
            VMEM((1, BATCH), jnp.int32),
            VMEM((PAGES, PAGE, HD), BF16),
            VMEM((8, BATCH), F32),
            VMEM((STEPS, 128), jnp.int32),
            pltpu.SemaphoreType.DMA((4,)),
            pltpu.SemaphoreType.DMA((2,)),
            *GATHER_SEMS,
        ],
        compiler_params=pltpu.CompilerParams(collective_id=0, has_side_effects=True, vmem_limit_bytes=12 << 20),
        name="prepare",
    )(q, table, counts, cache)


def attend_kernel(pick_in, who_in, q_in, kt, v, found, q, scores, pick, who, sems):
    tables = [pltpu.make_async_copy(pick_in, pick, sems.at[0]), pltpu.make_async_copy(who_in, who, sems.at[1])]
    for table in tables:
        table.start()

    def widen(i, carry):
        for j in range(4):
            q[pl.ds((i * 4 + j) * ROWS, ROWS)] = q_in[i * 4 + j].astype(F32).reshape(ROWS, HEADS, HD)
        return carry

    lax.fori_loop(0, BLOCKS // 4, widen, 0)
    found[pl.ds(NONE, 8), 0] = jnp.zeros((8, HEADS, HD), F32)
    found[pl.ds(NONE, 8), 1] = jnp.full((8, HEADS, HD), -1e30, F32)
    ones = jnp.ones((PAGE, HD), BF16)
    for table in tables:
        table.wait()

    def scores_of(g):
        for u in range(UNROLL):
            left = jnp.concatenate([q[who[g, u * CHUNK + j]] for j in range(CHUNK)], axis=0).astype(BF16)
            scores[u] = dot(left, kt[who[g, 64 + u]])

    def weigh(g):
        for u in range(UNROLL):
            at = pl.ds((g * UNROLL + u) * CHUNK, CHUNK)
            s = scores[u] * LOG2E_SCALE
            m = jnp.max(s, axis=1, keepdims=True)
            w = jnp.exp2(s - m).astype(BF16)
            o = dot(w, jnp.concatenate([v[who[g, 64 + u]], ones], axis=1))
            total = o[:, HD:]
            found[at, 0] = (o[:, :HD] / total).reshape(CHUNK, HEADS, HD)
            found[at, 1] = (m + jnp.log2(total)).reshape(CHUNK, HEADS, HD)

    scores_of(0)
    steps = (pick[0, CAP * ROWS] + UNROLL - 1) // UNROLL

    def step(g, carry):
        weigh(g)
        scores_of(jnp.minimum(g + 1, STEPS - 1))
        return carry

    lax.fori_loop(0, steps, step, 0)


def attend(pick, who, q, kt, v):
    vmem = pl.BlockSpec(memory_space=VMEM)
    return pl.pallas_call(
        attend_kernel,
        out_shape=VMEM((NONE + 8, 2, HEADS, HD), F32),
        in_specs=[vmem] * 5,
        out_specs=vmem,
        scratch_shapes=[
            VMEM((BATCH, HEADS, HD), F32),
            VMEM((UNROLL, CHUNK * HEADS, PAGE), F32),
            pltpu.SMEM((BLOCKS, 128), jnp.int32),
            pltpu.SMEM((STEPS, 128), jnp.int32),
            pltpu.SemaphoreType.DMA((2,)),
        ],
        compiler_params=pltpu.CompilerParams(vmem_limit_bytes=8 << 20),
        name="attend",
    )(pick, who, q, kt, v)


def settle(pick, found, g, values, stats):
    sublane = lax.broadcasted_iota(jnp.int32, (HEADS, HD), 0)
    lane = lax.broadcasted_iota(jnp.int32, (HEADS, HD), 1)
    tops = jnp.zeros((HEADS, HD), F32)
    totals = jnp.zeros((HEADS, HD), F32)
    outs = []
    for s in range(ROWS):
        at = [pick[g, k * ROWS + s] for k in range(CAP)]
        highest = [found[p, 1] for p in at]
        m = jnp.maximum(jnp.floor(functools.reduce(jnp.maximum, highest) * 0.5 + 0.5) * 2.0, LOWEST)
        factors = [jnp.exp2(t - m) for t in highest]
        outs.append(sum(f * found[p, 0] for f, p in zip(factors, at)))
        here = lane - sublane == s * HEADS
        tops = jnp.where(here, m, tops)
        totals = jnp.where(here, sum(factors), totals)
    stats[0:1] = jnp.sum(tops, axis=0, keepdims=True)
    stats[1:2] = jnp.sum(totals, axis=0, keepdims=True)
    values[...] = jnp.concatenate(outs, axis=0).astype(BF16)


def merge(parts, stats, diagonal):
    m = functools.reduce(jnp.maximum, [s[0:1] for s in stats])
    factors = [jnp.exp2(s[0:1] - m) for s in stats]
    total = sum(s[1:2] * f for s, f in zip(stats, factors))
    left = jnp.concatenate([jnp.where(diagonal, jnp.broadcast_to(f, (TILE, TILE)), 0.0).astype(BF16) for f in factors], axis=1)
    return dot(left, jnp.concatenate(parts, axis=0)), m, total


def finish_kernel(
    pick, found, w_ref, out_ref,
    own_acc, own_stats, their_acc, their_stats,
    core_acc, core_stats, y_out, y_out_stats, y_in, y_in_stats, z_out, z_out_stats, z_in, z_in_stats,
    turned, att, w, part, parts_in, w_sem,
    c_send, c_recv, cs_send, cs_recv, y_send, y_recv, ys_send, ys_recv, z_send, z_recv, zs_send, zs_recv, h_send, h_recv, *sems,
):
    y, z, c = position()
    h = lax.axis_index("head")
    other = 1 - c
    load_w = pltpu.make_async_copy(w_ref, w, w_sem)
    load_w.start()
    partner = at_seq(y, z, other)
    order = (2, 1, 3, 0)

    def settle_all(e, core, values, stats):
        def one(yy, carry):
            settle(pick, found, (yy * Z + (z + e) % Z) * C + core, values.at[e, yy], stats.at[e, yy])
            return carry

        lax.fori_loop(0, Y, one, 0)

    def early():
        for e in order:
            settle_all(e, other, their_acc, their_stats)
        settle_all(order[0], c, own_acc, own_stats)

    greet(seq_peers(y, z, c) + [{"head": (h + d) % GROUPS} for d in range(1, GROUPS)], early)
    copies = []
    for e in order:
        copies.append(send(their_acc.at[e], core_acc.at[e], c_send.at[e], c_recv.at[e], partner))
        copies.append(send(their_stats.at[e], core_stats.at[e], cs_send.at[e], cs_recv.at[e], partner))
    diagonal = lax.broadcasted_iota(jnp.int32, (TILE, TILE), 0) == lax.broadcasted_iota(jnp.int32, (TILE, TILE), 1)

    def put(values, rows, o, m, total):
        values[...] = o.astype(BF16)
        rows[0:1] = m
        rows[1:2] = total

    for e in order:
        if e != order[0]:
            settle_all(e, c, own_acc, own_stats)
        arrived(core_acc.at[e], c_send.at[e], c_recv.at[e], partner)
        arrived(core_stats.at[e], cs_send.at[e], cs_recv.at[e], partner)
        for d in order:
            yy = (y + d) % Y
            merged = merge([own_acc[e, yy], core_acc[e, yy]], [own_stats[e, yy], core_stats[e, yy]], diagonal)
            if d == 0:
                put(y_in.at[0, e], y_in_stats.at[0, e], *merged)
            else:
                put(y_out.at[d, e], y_out_stats.at[d, e], *merged)
                there = at_seq(yy, z, c)
                copies.append(send(y_out.at[d, e], y_in.at[d, e], y_send.at[d, e], y_recv.at[d, e], there))
                copies.append(send(y_out_stats.at[d, e], y_in_stats.at[d, e], ys_send.at[d, e], ys_recv.at[d, e], there))
    for e in order:
        for d in (1, 3, 2):
            there = at_seq((y - d + Y) % Y, z, c)
            arrived(y_in.at[d, e], y_send.at[d, e], y_recv.at[d, e], there)
            arrived(y_in_stats.at[d, e], ys_send.at[d, e], ys_recv.at[d, e], there)
        merged = merge([y_in[d, e] for d in range(Y)], [y_in_stats[d, e] for d in range(Y)], diagonal)
        if e == 0:
            put(z_in.at[0], z_in_stats.at[0], *merged)
        else:
            put(z_out.at[e], z_out_stats.at[e], *merged)
            there = at_seq(y, (z + e) % Z, c)
            copies.append(send(z_out.at[e], z_in.at[e], z_send.at[e], z_recv.at[e], there))
            copies.append(send(z_out_stats.at[e], z_in_stats.at[e], zs_send.at[e], zs_recv.at[e], there))
    for e in (2, 1, 3):
        there = at_seq(y, (z - e + Z) % Z, c)
        arrived(z_in.at[e], z_send.at[e], z_recv.at[e], there)
        arrived(z_in_stats.at[e], zs_send.at[e], zs_recv.at[e], there)
    o, m, total = merge([z_in[e] for e in range(Z)], [z_in_stats[e] for e in range(Z)], diagonal)
    turned[...] = o / jnp.broadcast_to(total, (TILE, TILE)).T
    for i in range(HEADS):
        att[y, z, c, :, i * HD : (i + 1) * HD] = turned[pl.ds(i, ROWS, stride=HEADS), :].astype(BF16)
    gather = Gather(att, *sems)
    gather.start()
    for copy in copies:
        copy.wait_send()
    load_w.wait()
    near = 3 - 2 * (z % 2)
    far = Z - near
    for dy in (1, 3):
        gather.from_y(dy, 0)
    gather.from_z(near)
    gather.from_z(far)
    gather.from_y(2, 0)

    def exchange(to, pair):
        return pltpu.make_async_remote_copy(
            src_ref=part.at[to, pair], dst_ref=parts_in.at[h, pair], send_sem=h_send.at[to, pair], recv_sem=h_recv.at[h, pair],
            device_id={"head": to}, device_id_type=pl.DeviceIdType.MESH,
        )

    def project(dz):
        zz = (z - dz + Z) % Z
        pair = zz % 2
        rows = jnp.concatenate([att[yy, zz, j] for yy in range(Y) for j in range(C)], axis=0)
        share = dot(rows, w[...]).astype(BF16)
        for yy in range(Y):
            to = yy * 2 + zz // 2
            its = share[yy * C * ROWS : (yy + 1) * C * ROWS]

            @pl.when(to == h)
            def _():
                parts_in[h, pair] = its

            @pl.when(to != h)
            def _():
                part[to, pair] = its
                exchange(to, pair).start()

    gather.from_z(2)
    for dy in range(Y):
        gather.from_core(dy, 0)
    project(0)
    for dz in (near, far):
        for dy in (1, 3, 2):
            gather.from_y(dy, dz)
    for dy in range(Y):
        gather.from_core(dy, near)
    project(near)
    for dy in (1, 3, 2):
        gather.from_y(dy, 2)
    for dy in range(Y):
        gather.from_core(dy, far)
    project(far)
    for dy in range(Y):
        gather.from_core(dy, 2)
    project(2)
    gather.finish()
    for s in range(GROUPS):

        @pl.when(s != h)
        def _():
            for pair in range(2):
                arrived(parts_in.at[s, pair], h_send.at[s, pair], h_recv.at[s, pair], {"head": s})

    total = sum(parts_in[s].astype(F32) for s in range(GROUPS))
    out_ref[...] = total.reshape(out_ref.shape).astype(BF16)
    for s in range(GROUPS):

        @pl.when(s != h)
        def _():
            for pair in range(2):
                exchange(s, pair).wait_send()


def finish(pick, found, w):
    vmem = pl.BlockSpec(memory_space=VMEM)
    width = w.shape[1]
    rows = BATCH // GROUPS
    dma = pltpu.SemaphoreType.DMA
    return pl.pallas_call(
        finish_kernel,
        out_shape=jax.ShapeDtypeStruct((rows, width), BF16),
        in_specs=[pl.BlockSpec(memory_space=pltpu.SMEM), vmem, pl.BlockSpec(memory_space=pltpu.HBM)],
        out_specs=vmem,
        scratch_shapes=[
            VMEM((Z, Y, TILE, HD), BF16), VMEM((Z, Y, 2, HD), F32),
            VMEM((Z, Y, TILE, HD), BF16), VMEM((Z, Y, 2, HD), F32),
            VMEM((Z, Y, TILE, HD), BF16), VMEM((Z, Y, 2, HD), F32),
            VMEM((Y, Z, TILE, HD), BF16), VMEM((Y, Z, 2, HD), F32),
            VMEM((Y, Z, TILE, HD), BF16), VMEM((Y, Z, 2, HD), F32),
            VMEM((Z, TILE, HD), BF16), VMEM((Z, 2, HD), F32),
            VMEM((Z, TILE, HD), BF16), VMEM((Z, 2, HD), F32),
            VMEM((TILE, HD), F32),
            VMEM((Y, Z, C, ROWS, HEADS * HD), BF16),
            VMEM((HEADS * HD, width), BF16),
            VMEM((GROUPS, 2, rows // 2, width), BF16), VMEM((GROUPS, 2, rows // 2, width), BF16),
            dma,
            *[dma((Z,)) for _ in range(4)],
            *[dma((Y, Z)) for _ in range(4)],
            *[dma((Z,)) for _ in range(4)],
            dma((GROUPS, 2)), dma((GROUPS, 2)),
            *GATHER_SEMS,
        ],
        compiler_params=pltpu.CompilerParams(collective_id=1, has_side_effects=True, vmem_limit_bytes=12 << 20),
        name="finish",
    )(pick, found, w)


def shards(queries, cache, page_table, page_count, out_weight):
    cache = cache.reshape(2, PAGES, PAGE, HD)
    stay = functools.partial(pltpu.with_memory_space_constraint, memory_space=pltpu.HBM)
    q, pick, who, kt, v = prepare(stay(queries.reshape(TILE, HD)), stay(page_table.T), stay(page_count.reshape(1, BATCH)), stay(cache))
    found = attend(pick, who, q.reshape(BLOCKS, TILE, HD), kt, v)
    return finish(pick, found, stay(out_weight))


def solution(mesh):
    return jax.shard_map(
        shards,
        mesh=mesh,
        in_specs=(
            P("seq", "head", None),
            P(None, "seq", "head", None, None),
            P(),
            P(),
            P("head", "seq"),
        ),
        out_specs=P("head", "seq"),
        check_vma=False,
    )
```
